16 devices in a mesh: ep: 16 (over z, y, x, core).
Axes of the slice: x: 2, y: 2, z: 2, core: 2. Of those that a mesh axis runs over, the one named last changes fastest.
Arguments:
- tokens: bfloat16 [16, 256, 768], P('ep')
- loss_weight: bfloat16 [16, 256, 768], P('ep')
- w_gate: bfloat16 [768, 16], replicated
- w_in: bfloat16 [16, 768, 3072], P('ep')
- w_out: bfloat16 [16, 3072, 768], P('ep')
- first_expert: int32 [16, 256], P('ep')
- second_expert: int32 [16, 256], P('ep')
- keep_second: int32 [16, 256], P('ep')
Outputs:
- output 1: float32 [], replicated
- output 2: bfloat16 [16, 256, 768], P('ep')
- output 3: bfloat16 [16, 768, 3072], P('ep')
- output 4: bfloat16 [16, 3072, 768], P('ep')
- output 5: float32 [768, 16], replicated
All inputs are finite; a program needn't handle non-finite values.
Results may differ from the reference program's by a relative error of at most 0.00963735.
Values are sent between devices in bfloat16 or wider.
A program may use at most 1 GiB of HBM per device.

```python
import jax
import jax.numpy as jnp
from jax import lax

EXPERTS = 16
HIDDEN = 768
FF_DIM = 3072
SEQ_LEN = 256
GROUPS = 16
CAPACITY = 2 * SEQ_LEN // EXPERTS
TOKENS = GROUPS * SEQ_LEN
NUMEL = TOKENS * HIDDEN
ALPHA = 0.01


def draw_routes(route_key):
    sub_keys = jax.random.split(route_key, 6)
    skew_level = jax.random.randint(sub_keys[0], (GROUPS, 1), 0, 4)
    hot_expert = jax.random.randint(sub_keys[1], (GROUPS, 1), 0, EXPERTS)
    hot_pick = jax.random.randint(sub_keys[2], (GROUPS, SEQ_LEN), 0, 8)
    spread = jax.random.randint(sub_keys[3], (GROUPS, SEQ_LEN), 0, EXPERTS)
    first_expert = jnp.where(hot_pick < skew_level, hot_expert, spread).astype(jnp.int32)
    offset = jax.random.randint(sub_keys[4], (GROUPS, SEQ_LEN), 1, EXPERTS)
    second_expert = ((first_expert + offset) % EXPERTS).astype(jnp.int32)
    keep_second = (jax.random.randint(sub_keys[5], (GROUPS, SEQ_LEN), 0, 3) > 0).astype(jnp.int32)
    return first_expert, second_expert, keep_second


def setup_inputs(seed: int = 0) -> dict:
    sub_keys = jax.random.split(jax.random.key(seed), 6)
    tokens = jax.random.normal(sub_keys[0], (GROUPS, SEQ_LEN, HIDDEN), jnp.float32).astype(jnp.bfloat16)
    loss_weight = jax.random.normal(sub_keys[1], (GROUPS, SEQ_LEN, HIDDEN), jnp.float32).astype(jnp.bfloat16)
    w_gate = (jax.random.normal(sub_keys[2], (HIDDEN, EXPERTS), jnp.float32) * HIDDEN ** -0.5).astype(jnp.bfloat16)
    w_in = (jax.random.normal(sub_keys[3], (EXPERTS, HIDDEN, FF_DIM), jnp.float32) * HIDDEN ** -0.5).astype(jnp.bfloat16)
    w_out = (jax.random.normal(sub_keys[4], (EXPERTS, FF_DIM, HIDDEN), jnp.float32) * FF_DIM ** -0.5).astype(jnp.bfloat16)
    first_expert, second_expert, keep_second = draw_routes(sub_keys[5])
    return {'tokens': tokens, 'loss_weight': loss_weight, 'w_gate': w_gate, 'w_in': w_in, 'w_out': w_out, 'first_expert': first_expert, 'second_expert': second_expert, 'keep_second': keep_second}


def table_for(hot_rows, pos_rows, kept_rows):
    slot_ids = jnp.arange(CAPACITY, dtype=jnp.int32)
    slot_hit = ((pos_rows[:, None, None] == slot_ids) & (kept_rows[:, None, None] > 0)).astype(jnp.float32)
    return hot_rows[:, :, None] * slot_hit


def expert_apply(packed):
    x_slots, w_first, w_second = packed
    pre_act = jnp.einsum('gch,hf->gcf', x_slots.astype(jnp.float32), w_first.astype(jnp.float32))
    act_bf = jax.nn.gelu(pre_act, approximate=True).astype(jnp.bfloat16)
    return jnp.einsum('gcf,fh->gch', act_bf.astype(jnp.float32), w_second.astype(jnp.float32)).astype(jnp.bfloat16)


def reference(tokens, loss_weight, w_gate, w_in, w_out, first_expert, second_expert, keep_second):
    expert_ids = jnp.arange(EXPERTS, dtype=jnp.int32)
    first_int = (first_expert[..., None] == expert_ids).astype(jnp.int32)
    second_int = (second_expert[..., None] == expert_ids).astype(jnp.int32)
    second_keep = second_int * keep_second[..., None]
    first_count = jnp.sum(first_int, axis=1)
    pos_first = jnp.sum((jnp.cumsum(first_int, axis=1) - first_int) * first_int, axis=-1)
    pos_second = jnp.sum((jnp.cumsum(second_keep, axis=1) - second_keep + first_count[:, None, :]) * second_int, axis=-1)
    kept_first = (pos_first < CAPACITY).astype(jnp.int32)
    kept_second = keep_second * (pos_second < CAPACITY).astype(jnp.int32)
    first_hot = first_int.astype(jnp.float32)
    second_hot = second_int.astype(jnp.float32)
    frac_first = jnp.sum(first_hot, axis=(0, 1)) / TOKENS

    def dispatch_group(packed):
        x_group, pos_one, kept_one, hot_one, pos_two, kept_two, hot_two = packed
        table = table_for(hot_one, pos_one, kept_one) + table_for(hot_two, pos_two, kept_two)
        return jnp.einsum('sec,sh->ech', table, x_group).astype(jnp.bfloat16)

    def combine_group(packed):
        y_group, pos_one, kept_one, hot_one, pos_two, kept_two, hot_two, norm_one, norm_two = packed
        combine = (table_for(hot_one, pos_one, kept_one) * norm_one[:, None, None] + table_for(hot_two, pos_two, kept_two) * norm_two[:, None, None]).astype(jnp.bfloat16)
        return jnp.einsum('sec,ech->sh', combine.astype(jnp.float32), y_group.astype(jnp.float32))

    def objective(x_in, gate_w, w_first, w_second):
        x_f32 = x_in.astype(jnp.float32)
        logits = jnp.einsum('gsh,he->gse', x_f32, gate_w)
        router_prob = jax.nn.softmax(logits, axis=-1)
        gate_first = jnp.sum(router_prob * first_hot, axis=-1)
        gate_second = jnp.sum(router_prob * second_hot, axis=-1)
        norm_first = gate_first / (gate_first + gate_second)
        norm_second = gate_second / (gate_first + gate_second)
        slots_in = lax.map(jax.checkpoint(dispatch_group), (x_f32, pos_first, kept_first, first_hot, pos_second, kept_second, second_hot))
        slots_out = lax.map(jax.checkpoint(expert_apply), (jnp.moveaxis(slots_in, 0, 1), w_first, w_second))
        moe_out = lax.map(jax.checkpoint(combine_group), (jnp.moveaxis(slots_out, 0, 1), pos_first, kept_first, first_hot, pos_second, kept_second, second_hot, norm_first, norm_second))
        dot_sum = jnp.sum((x_f32 + moe_out) * loss_weight.astype(jnp.float32))
        mean_prob = jnp.sum(router_prob, axis=(0, 1)) / TOKENS
        loss_value = dot_sum / NUMEL + ALPHA * EXPERTS * jnp.sum(frac_first * mean_prob)
        return loss_value * NUMEL, loss_value

    _, pull_back, loss_value = jax.vjp(objective, tokens, w_gate.astype(jnp.float32), w_in, w_out, has_aux=True)
    grad_x, grad_gate, grad_w_in, grad_w_out = pull_back(jnp.ones((), jnp.float32))
    return loss_value, grad_x, grad_w_in, grad_w_out, grad_gate
```

```python
import functools

import jax
import jax.numpy as jnp
from jax import lax
from jax.experimental import pallas as pl
from jax.experimental.pallas import tpu as pltpu
from jax.sharding import PartitionSpec as P

ALPHA = 0.01
MESH = pl.DeviceIdType.MESH
F32 = jnp.float32
BF16 = jnp.bfloat16

DEVS = 16
LANES = 128
PAD = 8
HALF = 8

SEND_X, SEND_R, SEND_MSG, SEND_DOT, SEND_GX, SEND_RS, SEND_AG = range(7)


def offset_of(p):
    x, y = (p >> 1) & 1, (p >> 2) & 1
    z = x ^ y ^ ((p >> 3) & 1)
    return (p & 1) | (x << 1) | (y << 2) | (z << 3)


def block_of(ids, me):
    k = jnp.bitwise_xor(ids, me)
    parity = (k >> 1) ^ (k >> 2) ^ (k >> 3)
    return (k & 7) + 8 * (parity & 1)


def dot(a, b, ca=1, cb=0):
    return lax.dot_general(a, b, (((ca,), (cb,)), ((), ())), preferred_element_type=F32)


def iota(shape, axis):
    return lax.broadcasted_iota(jnp.int32, shape, axis)


def where(mask, value):
    return jnp.where(mask, value, jnp.zeros_like(value))


def tree_sum(rows):
    rows = list(rows)
    while len(rows) > 1:
        rows = [rows[i] + rows[i + 1] for i in range(0, len(rows), 2)]
    return rows[0]


def rows_of(ref, n, width=LANES):
    out = jnp.zeros((n, width), F32)
    sub = iota((n, width), 0)
    for i in range(n):
        out = jnp.where(sub == i, jnp.broadcast_to(ref[i], (n, width)), out)
    return out


def layer_kernel(cap, x_hbm, r_hbm, wg_hbm, w1_hbm, w2_hbm, e1_hbm, e2_hbm, k2_hbm,
                 loss_ref, gx_ref, dw1_ref, dw2_ref, gw_ref,
                 x, r, wg, w1, w2, ids, disp, xs, rs, xe, re, gy, act, slope, dpre, ybuf, gxs, gxb, xet,
                 msg_s, msg_r, dot_s, dot_r, red_s, red_r, row_s, row_r,
                 local_sem, send_sem, recv_sem):
    seq, hidden = x.shape
    ff = w1.shape[1]
    half = HALF * cap
    tokens_all = DEVS * seq
    numel = tokens_all * hidden

    me = lax.axis_index("ep")
    bits = [lax.rem(me // (1 << i), 2) for i in range(4)]

    def peer(p):
        k = offset_of(p)
        return sum(((1 - bits[i]) if (k >> i) & 1 else bits[i]) * (1 << i) for i in range(4))

    def remote(kind, p, src, dst):
        return pltpu.make_async_remote_copy(
            src_ref=src, dst_ref=dst, send_sem=send_sem.at[kind, p], recv_sem=recv_sem.at[kind, p],
            device_id=(peer(p),), device_id_type=MESH)

    others = range(1, DEVS)

    loads = [pltpu.make_async_copy(src, dst, local_sem.at[i]) for i, (src, dst) in enumerate((
        (e1_hbm, ids.at[0]), (e2_hbm, ids.at[1]), (k2_hbm, ids.at[2]), (x_hbm, x), (r_hbm, r),
        (wg_hbm, wg), (w1_hbm, w1), (w2_hbm, w2)))]
    for copy in loads:
        copy.start()
    barrier = pltpu.get_barrier_semaphore()
    for p in others:
        pl.semaphore_signal(barrier, inc=1, device_id=(peer(p),), device_id_type=MESH)

    for i in range(3):
        loads[i].wait()
    e1, e2, k2 = ids[0], ids[1], ids[2]
    expert = iota((DEVS, seq), 0)
    hot1 = (e1 == expert).astype(F32)
    hot2 = (e2 == expert).astype(F32)
    kept2 = hot2 * k2.astype(F32)
    earlier = (iota((seq, seq), 0) < iota((seq, seq), 1)).astype(F32).astype(BF16)
    before = dot(jnp.concatenate([hot1, kept2], axis=0).astype(BF16), earlier)
    count1 = jnp.sum(hot1, axis=1, keepdims=True)
    pos1 = jnp.sum(before[:DEVS] * hot1, axis=0, keepdims=True).astype(jnp.int32)
    pos2 = jnp.sum((before[DEVS:] + count1) * hot2, axis=0, keepdims=True).astype(jnp.int32)
    keep1 = pos1 < cap
    keep2 = (pos2 < cap) & (k2 > 0)
    block1, block2 = block_of(e1, me), block_of(e2, me)
    slot1 = jnp.where(keep1, block1 * cap + pos1, -1)
    slot2 = jnp.where(keep2, block2 * cap + pos2, -1)

    loads[3].wait()
    for c in range(2):
        rows = pl.ds(c * half, half)
        slot = iota((half, seq), 0) + c * half
        table = ((slot == slot1) | (slot == slot2)).astype(F32).astype(BF16)
        disp[rows, :] = table
        xs[rows, :] = dot(table, x[...]).astype(BF16)
    pl.semaphore_wait(barrier, DEVS - 1)
    blk = lambda ref, p: ref.at[pl.ds(p * cap, cap), :]
    copies_x = {p: remote(SEND_X, p, blk(xs, p), blk(xe, p)) for p in others}
    for p in others:
        copies_x[p].start()
    xe[pl.ds(0, cap), :] = xs[pl.ds(0, cap), :]

    loads[4].wait()
    for c in range(2):
        rows = pl.ds(c * half, half)
        rs[rows, :] = dot(disp[rows, :], r[...]).astype(BF16)
    loads[5].wait()
    logits = dot(wg[...], x[...], 1, 1)
    shifted = jnp.exp(logits - jnp.max(logits, axis=0, keepdims=True))
    prob = shifted / jnp.sum(shifted, axis=0, keepdims=True)
    gate1 = jnp.sum(prob * hot1, axis=0, keepdims=True)
    gate2 = jnp.sum(prob * hot2, axis=0, keepdims=True)
    gate_sum = gate1 + gate2
    norm1 = (gate1 / gate_sum).astype(BF16).astype(F32)
    norm2 = (gate2 / gate_sum).astype(BF16).astype(F32)
    place = iota((LANES, seq), 0)
    at1 = (place == jnp.where(keep1, pos1, -1)).astype(F32).astype(BF16)
    at2 = (place == jnp.where(keep2, pos2, -1)).astype(F32).astype(BF16)
    weights = dot((hot1 * norm1).astype(BF16), at1, 1, 1) + dot((hot2 * norm2).astype(BF16), at2, 1, 1)
    prob_sum = jnp.sum(prob, axis=1, keepdims=True)
    sub, lane = iota((DEVS, LANES), 0), iota((DEVS, LANES), 1)
    stats = where(lane == sub + cap, jnp.broadcast_to(count1, (DEVS, LANES)))
    stats += where(lane == sub + cap + DEVS, jnp.broadcast_to(prob_sum, (DEVS, LANES)))
    message = weights + jnp.sum(stats, axis=0, keepdims=True)
    for e in range(DEVS):
        msg_s[e] = message[e:e + 1]
    msg_r[0] = msg_s[me]
    copies_msg = {p: remote(SEND_MSG, p, msg_s.at[peer(p)], msg_r.at[p]) for p in others}
    copies_r = {p: remote(SEND_R, p, blk(rs, p), blk(re, p)) for p in others}
    for p in others:
        copies_msg[p].start()
    for p in others:
        copies_r[p].start()
    re[pl.ds(0, cap), :] = rs[pl.ds(0, cap), :]

    loads[6].wait()
    loads[7].wait()
    wide = 512
    for c in range(2):
        rows = pl.ds(c * half, half)
        for p in range(c * HALF, (c + 1) * HALF):
            if p:
                copies_x[p].wait_recv()

        @pl.loop(0, ff // wide)
        def _(n):
            cols = pl.ds(pl.multiple_of(n * wide, wide), wide)
            pre = dot(xe[rows, :], w1[:, cols])
            sq = pre * pre
            root = 0.7978845608028654
            t = jnp.tanh(pre * (root + root * 0.044715 * sq))
            hx = 0.5 * pre
            act[rows, cols] = (hx + hx * t).astype(BF16)
            slope[rows, cols] = (0.5 + 0.5 * t) + hx * (1.0 - t * t) * (root + 3.0 * root * 0.044715 * sq)

        @pl.loop(0, hidden // 256)
        def _(n):
            cols = pl.ds(pl.multiple_of(n * 256, 256), 256)
            ybuf[rows, cols] = dot(act[rows, :], w2[:, cols]).astype(BF16)

    copies_dot, copies_gx = {}, {}
    for c in range(2):
        rows = pl.ds(c * half, half)
        mine = range(c * HALF, (c + 1) * HALF)
        for p in mine:
            if p:
                copies_msg[p].wait_recv()
                copies_r[p].wait_recv()
        diag = iota((half, LANES), 1) == lax.rem(iota((half, LANES), 0), cap)
        spread = jnp.concatenate([jnp.broadcast_to(msg_r[p], (cap, LANES)) for p in mine], axis=0)
        weight = jnp.sum(where(diag, spread), axis=1, keepdims=True)
        r_rows = re[rows, :].astype(F32)
        gy[rows, :] = (r_rows * weight).astype(BF16)
        dots = jnp.sum(r_rows * ybuf[rows, :].astype(F32), axis=1, keepdims=True)
        dot_mat = where(diag, jnp.broadcast_to(dots, (half, LANES)))
        for p in mine:
            q = (p - c * HALF) * cap
            row = jnp.sum(dot_mat[q:q + cap], axis=0, keepdims=True)
            if p:
                dot_s[p] = row
            else:
                dot_r[p] = row

        @pl.loop(0, ff // wide)
        def _(n):
            cols = pl.ds(pl.multiple_of(n * wide, wide), wide)
            da = dot(gy[rows, :], w2[cols, :], 1, 1).astype(BF16).astype(F32)
            dpre[rows, cols] = (da * slope[rows, cols]).astype(BF16)

        for p in mine:
            if p:
                copies_dot[p] = remote(SEND_DOT, p, dot_s.at[p], dot_r.at[p])
                copies_dot[p].start()

        @pl.loop(0, hidden // 256)
        def _(n):
            cols = pl.ds(pl.multiple_of(n * 256, 256), 256)
            gxs[rows, cols] = dot(dpre[rows, :], w1[cols, :], 1, 1).astype(BF16)

        xet[:, rows] = jnp.transpose(xe[rows, :])
        for p in mine:
            if p:
                copies_gx[p] = remote(SEND_GX, p, blk(gxs, p), blk(gxb, p))
                copies_gx[p].start()
            else:
                gxb[pl.ds(0, cap), :] = gxs[pl.ds(0, cap), :]

    totals = tree_sum([msg_r[p] for p in range(DEVS)])
    spread = jnp.broadcast_to(totals, (DEVS, LANES))
    count_all = jnp.sum(where(lane == sub + cap, spread), axis=1, keepdims=True)
    prob_all = jnp.sum(where(lane == sub + cap + DEVS, spread), axis=1, keepdims=True)
    frac = count_all * (1.0 / tokens_all)
    for p in others:
        copies_dot[p].wait_recv()
    dots = rows_of(dot_r, DEVS)
    dots_bf = dots.astype(BF16)
    found1 = dot(dots_bf, at1)
    found2 = dot(dots_bf, at2)
    grad1 = jnp.sum(where(block1 == expert, found1), axis=0, keepdims=True)
    grad2 = jnp.sum(where(block2 == expert, found2), axis=0, keepdims=True)
    inv_sq = 1.0 / (gate_sum * gate_sum)
    dgate1 = (grad1 - grad2) * gate2 * inv_sq
    dgate2 = (grad2 - grad1) * gate1 * inv_sq
    dprob = dgate1 * hot1 + dgate2 * hot2 + (ALPHA * hidden * DEVS) * frac
    dlogits = prob * (dprob - jnp.sum(prob * dprob, axis=0, keepdims=True))
    dlog_bf = dlogits.astype(BF16)
    grad_gate = dot(dlog_bf, x[...])
    own = jnp.sum(jnp.sum(x[...].astype(F32) * r[...].astype(F32), axis=0, keepdims=True), axis=1, keepdims=True)
    moe = jnp.sum(norm1 * jnp.sum(where(block1 == expert, dot_f32(dots, at1)), axis=0, keepdims=True)
                  + norm2 * jnp.sum(where(block2 == expert, dot_f32(dots, at2)), axis=0, keepdims=True),
                  axis=1, keepdims=True)
    part = jnp.broadcast_to(own + moe, (DEVS, LANES))
    reduced = jnp.concatenate([grad_gate, part], axis=1)
    for e in range(DEVS):
        red_s[e] = reduced[e:e + 1]
    red_r[0] = red_s[me]
    copies_rs = {p: remote(SEND_RS, p, red_s.at[peer(p)], red_r.at[p]) for p in others}
    for p in others:
        copies_rs[p].start()

    @pl.loop(0, ff // 256)
    def _(n):
        cols = pl.ds(pl.multiple_of(n * 256, 256), 256)
        dw2_ref[cols, :] = dot(act[:, cols], gy[...], 0, 0).astype(BF16)

    for p in others:
        copies_rs[p].wait_recv()
    total = tree_sum([red_r[p] for p in range(DEVS)])
    row_s[0] = total[:, :hidden]
    row_r[me] = total[:, :hidden]
    copies_ag = {p: remote(SEND_AG, p, row_s.at[0], row_r.at[me]) for p in others}
    dot_total = total[:, hidden:hidden + 1]
    aux = DEVS * jnp.sum(frac * (prob_all * (1.0 / tokens_all)), axis=0, keepdims=True)
    loss_ref[...] = jnp.broadcast_to(dot_total * (1.0 / numel) + ALPHA * aux, loss_ref.shape)
    for p in others:
        copies_ag[p].start()

    @pl.loop(0, ff // wide)
    def _(n):
        cols = pl.ds(pl.multiple_of(n * wide, wide), wide)
        dw1_ref[:, cols] = dot(xet[...], dpre[:, cols]).astype(BF16)

    dlog_pad = jnp.concatenate([dlogits, jnp.zeros((LANES - DEVS, seq), F32)], axis=0)
    gate_pad = jnp.concatenate([wg[...], jnp.zeros((LANES - DEVS, hidden), BF16)], axis=0)
    router = dot(jnp.transpose(dlog_pad).astype(BF16), gate_pad)
    base = r[...].astype(F32) + router
    for p in others:
        copies_gx[p].wait_recv()
    gx_ref[...] = (base + dot(disp[...], gxb[...], 0, 0)).astype(BF16)

    for p in others:
        copies_ag[p].wait_recv()
    gw_ref[...] = rows_of(row_r, DEVS, hidden)

    for group in (copies_x, copies_r, copies_msg, copies_dot, copies_gx, copies_rs, copies_ag):
        for p in others:
            group[p].wait_send()


def dot_f32(values, table):
    high = values.astype(BF16)
    rest = values - high.astype(F32)
    mid = rest.astype(BF16)
    low = (rest - mid.astype(F32)).astype(BF16)
    return dot(high, table) + dot(mid, table) + dot(low, table)


def store_kernel(loss, gx, dw1, dw2, gw, loss_out, gx_out, dw1_out, dw2_out, gw_out, sem):
    copies = [pltpu.make_async_copy(src, dst, sem.at[i]) for i, (src, dst) in enumerate((
        (dw1, dw1_out), (dw2, dw2_out), (gx, gx_out), (gw, gw_out)))]
    for copy in copies:
        copy.start()
    loss_out[0, 0] = jnp.max(loss[...])
    for copy in copies:
        copy.wait()


def solution(mesh):
    def layer_body(x_loc, r_loc, w_gate, w_in_loc, w_out_loc, first_ids, second_ids, keep_ids):
        _, seq, hidden = x_loc.shape
        ff = w_in_loc.shape[2]
        cap = 2 * seq // DEVS
        slots = DEVS * cap
        anyspace = pl.BlockSpec(memory_space=pl.ANY)
        vmem = pl.BlockSpec(memory_space=pltpu.VMEM)
        results = pl.pallas_call(
            functools.partial(layer_kernel, cap),
            out_shape=(
                pltpu.VMEM((8, LANES), F32),
                pltpu.VMEM((seq, hidden), BF16),
                pltpu.VMEM((hidden, ff), BF16),
                pltpu.VMEM((ff, hidden), BF16),
                pltpu.VMEM((DEVS, hidden), F32),
            ),
            in_specs=[anyspace] * 8,
            out_specs=(vmem,) * 5,
            scratch_shapes=[
                pltpu.VMEM((seq, hidden), BF16),
                pltpu.VMEM((seq, hidden), BF16),
                pltpu.VMEM((DEVS, hidden), BF16),
                pltpu.VMEM((hidden, ff), BF16),
                pltpu.VMEM((ff, hidden), BF16),
                pltpu.VMEM((3 + PAD, 1, seq), jnp.int32),
                pltpu.VMEM((slots, seq), BF16),
                pltpu.VMEM((slots, hidden), BF16),
                pltpu.VMEM((slots, hidden), BF16),
                pltpu.VMEM((slots, hidden), BF16),
                pltpu.VMEM((slots, hidden), BF16),
                pltpu.VMEM((slots, hidden), BF16),
                pltpu.VMEM((slots, ff), BF16),
                pltpu.VMEM((slots, ff), F32),
                pltpu.VMEM((slots, ff), BF16),
                pltpu.VMEM((slots, hidden), BF16),
                pltpu.VMEM((slots, hidden), BF16),
                pltpu.VMEM((slots, hidden), BF16),
                pltpu.VMEM((hidden, slots), BF16),
                pltpu.VMEM((DEVS + PAD, 1, LANES), F32),
                pltpu.VMEM((DEVS + PAD, 1, LANES), F32),
                pltpu.VMEM((DEVS + PAD, 1, LANES), F32),
                pltpu.VMEM((DEVS + PAD, 1, LANES), F32),
                pltpu.VMEM((DEVS + PAD, 1, hidden + LANES), F32),
                pltpu.VMEM((DEVS + PAD, 1, hidden + LANES), F32),
                pltpu.VMEM((1 + PAD, 1, hidden), F32),
                pltpu.VMEM((DEVS + PAD, 1, hidden), F32),
                pltpu.SemaphoreType.DMA((8,)),
                pltpu.SemaphoreType.DMA((7, DEVS)),
                pltpu.SemaphoreType.DMA((7, DEVS)),
            ],
            compiler_params=pltpu.CompilerParams(
                collective_id=0, has_side_effects=True, vmem_limit_bytes=48 * 1024 * 1024),
            name="moe_layer",
        )(x_loc[0], r_loc[0], w_gate.T, w_in_loc[0], w_out_loc[0], first_ids, second_ids, keep_ids)
        loss, gx, dw1, dw2, gw = pl.pallas_call(
            store_kernel,
            out_shape=(
                jax.ShapeDtypeStruct((1, 1), F32),
                jax.ShapeDtypeStruct((seq, hidden), BF16),
                jax.ShapeDtypeStruct((hidden, ff), BF16),
                jax.ShapeDtypeStruct((ff, hidden), BF16),
                jax.ShapeDtypeStruct((DEVS, hidden), F32),
            ),
            in_specs=[vmem] * 5,
            out_specs=(pl.BlockSpec(memory_space=pltpu.SMEM),) + (anyspace,) * 4,
            scratch_shapes=[pltpu.SemaphoreType.DMA((4,))],
            compiler_params=pltpu.CompilerParams(vmem_limit_bytes=2 * 1024 * 1024),
            name="store_results",
        )(*results)
        return loss.reshape(()), gx[None], dw1[None], dw2[None], gw.T

    row_spec = P('ep', None, None)
    id_spec = P('ep', None)
    return jax.shard_map(layer_body, mesh=mesh, in_specs=(row_spec, row_spec, P(None, None), row_spec, row_spec, id_spec, id_spec, id_spec), out_specs=(P(), row_spec, row_spec, row_spec, P(None, None)), check_vma=False)
```

```python
import functools

import jax
import jax.numpy as jnp
from jax import lax
from jax.experimental import pallas as pl
from jax.experimental.pallas import tpu as pltpu
from jax.sharding import PartitionSpec as P

ALPHA = 0.01
MESH = pl.DeviceIdType.MESH
F32 = jnp.float32
BF16 = jnp.bfloat16

DEVS = 16
LANES = 128
PAD = 8
HALF = 8

SEND_X, SEND_R, SEND_MSG, SEND_DOT, SEND_GX, SEND_RS, SEND_AG = range(7)


def offset_of(p):
    x, y = (p >> 1) & 1, (p >> 2) & 1
    z = x ^ y ^ ((p >> 3) & 1)
    return (p & 1) | (x << 1) | (y << 2) | (z << 3)


def block_of(ids, me):
    k = jnp.bitwise_xor(ids, me)
    parity = (k >> 1) ^ (k >> 2) ^ (k >> 3)
    return (k & 7) + 8 * (parity & 1)


def dot(a, b, ca=1, cb=0):
    return lax.dot_general(a, b, (((ca,), (cb,)), ((), ())), preferred_element_type=F32)


def iota(shape, axis):
    return lax.broadcasted_iota(jnp.int32, shape, axis)


def where(mask, value):
    return jnp.where(mask, value, jnp.zeros_like(value))


def tree_sum(rows):
    rows = list(rows)
    while len(rows) > 1:
        rows = [rows[i] + rows[i + 1] for i in range(0, len(rows), 2)]
    return rows[0]


def rows_of(ref, places, width):
    n = len(places)
    out = jnp.zeros((n, width), F32)
    sub = iota((n, width), 0)
    for i, place in enumerate(places):
        out = jnp.where(sub == place, jnp.broadcast_to(ref[i], (n, width)), out)
    return out


def split3(values):
    high = values.astype(BF16)
    rest = values - high.astype(F32)
    mid = rest.astype(BF16)
    return high, mid, (rest - mid.astype(F32)).astype(BF16)


def layer_kernel(cap, x_hbm, r_hbm, wg_hbm, w1_hbm, w2_hbm, e1_hbm, e2_hbm, k2_hbm,
                 loss_ref, gx_ref, dw1_ref, dw2_ref, gw_ref,
                 x, r, wg, w1, w2, ids, disp, dispt, xs, rs, xe, re, gy, pre, act, actt, acc, slope, dpre, ybuf, gxs, gxb, xet,
                 msg_s, msg_r, dot_s, dot_r, red_s, red_r, row_s, row_r,
                 local_sem, send_sem, recv_sem):
    seq, hidden = x.shape
    ff = w1.shape[1]
    half = HALF * cap
    tokens_all = DEVS * seq
    numel = tokens_all * hidden

    me = lax.axis_index("ep")
    bits = [lax.rem(me // (1 << i), 2) for i in range(4)]

    def peer(p):
        k = offset_of(p)
        return sum(((1 - bits[i]) if (k >> i) & 1 else bits[i]) * (1 << i) for i in range(4))

    def remote(kind, p, src, dst):
        return pltpu.make_async_remote_copy(
            src_ref=src, dst_ref=dst, send_sem=send_sem.at[kind], recv_sem=recv_sem.at[kind, p // HALF],
            device_id=(peer(p),), device_id_type=MESH)

    others = range(1, DEVS)
    halves = (range(1, HALF), range(HALF, DEVS))
    blk = lambda ref, p, n=1: ref.at[pl.ds(p * cap, n * cap), :]
    row = lambda ref, p, n=1: ref.at[pl.ds(p, n)]

    def wait_half(kind, c, part, ref):
        first, count = halves[c][0], len(halves[c])
        view = part(ref, first, count)
        remote(kind, first, view, view).wait_recv()

    id_copies = [pltpu.make_async_copy(src, ids.at[i], local_sem.at[0]) for i, src in enumerate((e1_hbm, e2_hbm, k2_hbm))]
    id_wait = pltpu.make_async_copy(row(ids, 0, 3), row(ids, 0, 3), local_sem.at[0])
    x_copy, r_copy, wg_copy, w1_copy, w2_copy = [
        pltpu.make_async_copy(src, dst, local_sem.at[1 + i]) for i, (src, dst) in enumerate((
            (x_hbm, x), (r_hbm, r), (wg_hbm, wg), (w1_hbm, w1), (w2_hbm, w2)))]
    barrier = pltpu.get_barrier_semaphore()
    for p in others:
        pl.semaphore_signal(barrier, inc=1, device_id=(peer(p),), device_id_type=MESH)
    for copy in id_copies + [x_copy, r_copy, wg_copy, w1_copy, w2_copy]:
        copy.start()

    expert = iota((DEVS, seq), 0)
    earlier = (iota((seq, seq), 0) < iota((seq, seq), 1)).astype(F32).astype(BF16)
    id_wait.wait()
    e1, e2, k2 = ids[0], ids[1], ids[2]
    hot1 = (e1 == expert).astype(F32)
    hot2 = (e2 == expert).astype(F32)
    kept2 = hot2 * k2.astype(F32)
    before = dot(jnp.concatenate([hot1, kept2], axis=0).astype(BF16), earlier)
    count1 = jnp.sum(hot1, axis=1, keepdims=True)
    pos1 = jnp.sum(before[:DEVS] * hot1, axis=0, keepdims=True).astype(jnp.int32)
    pos2 = jnp.sum((before[DEVS:] + count1) * hot2, axis=0, keepdims=True).astype(jnp.int32)
    keep1 = pos1 < cap
    keep2 = (pos2 < cap) & (k2 > 0)
    block1, block2 = block_of(e1, me), block_of(e2, me)
    slot1 = jnp.where(keep1, block1 * cap + pos1, -1)
    slot2 = jnp.where(keep2, block2 * cap + pos2, -1)

    half_rows = [pl.ds(c * half, half) for c in range(2)]

    def dispatch_x(c):
        slot = iota((half, seq), 0) + c * half
        table = ((slot == slot1) | (slot == slot2)).astype(F32).astype(BF16)
        disp[half_rows[c], :] = table
        xs[half_rows[c], :] = dot(table, x[...]).astype(BF16)

    def dispatch_r(c):
        rs[half_rows[c], :] = dot(disp[half_rows[c], :], r[...]).astype(BF16)

    def send_blocks(kind, c, src, dst):
        for p in halves[c]:
            remote(kind, p, blk(src, p), blk(dst, p)).start()

    x_copy.wait()
    dispatch_x(0)
    pl.semaphore_wait(barrier, DEVS - 1)
    send_blocks(SEND_X, 0, xs, xe)
    xe[pl.ds(0, cap), :] = xs[pl.ds(0, cap), :]
    r_copy.wait()
    dispatch_r(0)
    wg_copy.wait()
    logits = dot(wg[...], x[...], 1, 1)
    shifted = jnp.exp(logits - jnp.max(logits, axis=0, keepdims=True))
    prob = shifted / jnp.sum(shifted, axis=0, keepdims=True)
    gate1 = jnp.sum(prob * hot1, axis=0, keepdims=True)
    gate2 = jnp.sum(prob * hot2, axis=0, keepdims=True)
    gate_sum = gate1 + gate2
    norm1 = (gate1 / gate_sum).astype(BF16).astype(F32)
    norm2 = (gate2 / gate_sum).astype(BF16).astype(F32)
    place = iota((LANES, seq), 0)
    at1 = (place == jnp.where(keep1, pos1, -1)).astype(F32).astype(BF16)
    at2 = (place == jnp.where(keep2, pos2, -1)).astype(F32).astype(BF16)
    weights = dot((hot1 * norm1).astype(BF16), at1, 1, 1) + dot((hot2 * norm2).astype(BF16), at2, 1, 1)
    prob_sum = jnp.sum(prob, axis=1, keepdims=True)
    sub, lane = iota((DEVS, LANES), 0), iota((DEVS, LANES), 1)
    stats = where(lane == sub + cap, jnp.broadcast_to(count1, (DEVS, LANES)))
    stats += where(lane == sub + cap + DEVS, jnp.broadcast_to(prob_sum, (DEVS, LANES)))
    message = weights + jnp.sum(stats, axis=0, keepdims=True)
    for e in range(DEVS):
        msg_s[e] = message[e:e + 1]
    msg_r[0] = msg_s[me]
    for p in others:
        remote(SEND_MSG, p, msg_s.at[pl.ds(peer(p), 1)], row(msg_r, p)).start()
    send_blocks(SEND_R, 0, rs, re)
    re[pl.ds(0, cap), :] = rs[pl.ds(0, cap), :]
    dispatch_x(1)
    dispatch_r(1)
    send_blocks(SEND_X, 1, xs, xe)
    send_blocks(SEND_R, 1, rs, re)
    dispt[...] = jnp.transpose(disp[...])
    own = jnp.sum(jnp.sum(x[...].astype(F32) * r[...].astype(F32), axis=0, keepdims=True), axis=1, keepdims=True)

    wide = 512
    tiles = ff // wide
    tile = lambda n: pl.ds(n * wide, wide)
    diag = iota((half, LANES), 1) == lax.rem(iota((half, LANES), 0), cap)

    def forward(c):
        rows = half_rows[c]
        for n in range(tiles + 2):
            if n < tiles:
                pre[n % 2] = dot(xe[rows, :], w1[:, tile(n)])
            if 1 <= n <= tiles:
                m = n - 1
                v = pre[m % 2]
                sq = v * v
                root = 0.7978845608028654
                t = jnp.tanh(v * (root + root * 0.044715 * sq))
                hx = 0.5 * v
                a = (hx + hx * t).astype(BF16)
                act[rows, tile(m)] = a
                actt[tile(m), rows] = jnp.transpose(a)
                slope[rows, tile(m)] = (0.5 + 0.5 * t) + hx * (1.0 - t * t) * (root + 3.0 * root * 0.044715 * sq)
            if n >= 2:
                m = n - 2
                y = dot(act[rows, tile(m)], w2[tile(m), :])
                if m:
                    y += acc[...]
                if m < tiles - 1:
                    acc[...] = y
                else:
                    ybuf[rows, :] = y.astype(BF16)

    def cotangents(c):
        rows = half_rows[c]
        mine = range(c * HALF, (c + 1) * HALF)
        spread = jnp.concatenate([jnp.broadcast_to(msg_r[p], (cap, LANES)) for p in mine], axis=0)
        weight = jnp.sum(where(diag, spread), axis=1, keepdims=True)
        r_rows = re[rows, :].astype(F32)
        gy[rows, :] = (r_rows * weight).astype(BF16)
        dots = jnp.sum(r_rows * ybuf[rows, :].astype(F32), axis=1, keepdims=True)
        dot_mat = where(diag, jnp.broadcast_to(dots, (half, LANES)))
        for p in mine:
            q = (p - c * HALF) * cap
            (dot_s if p else dot_r)[p] = jnp.sum(dot_mat[q:q + cap], axis=0, keepdims=True)

    def slot_grads(c):
        rows = half_rows[c]
        for n in range(tiles):
            da = dot(gy[rows, :], w2[tile(n), :], 1, 1).astype(BF16).astype(F32)
            dpre[rows, tile(n)] = (da * slope[rows, tile(n)]).astype(BF16)

    def back_rows(c):
        rows = half_rows[c]
        for n in range(hidden // 256):
            cols = pl.ds(n * 256, 256)
            gxs[rows, cols] = dot(dpre[rows, :], w1[cols, :], 1, 1).astype(BF16)

    def send_dots(c):
        for p in halves[c]:
            remote(SEND_DOT, p, row(dot_s, p), row(dot_r, p)).start()

    def send_back(blocks):
        for p in blocks:
            remote(SEND_GX, p, blk(gxs, p), blk(gxb, p)).start()

    w1_copy.wait()
    w2_copy.wait()
    wait_half(SEND_X, 0, blk, xe)
    forward(0)
    wait_half(SEND_MSG, 0, row, msg_r)
    wait_half(SEND_R, 0, blk, re)
    cotangents(0)
    send_dots(0)
    slot_grads(0)
    back_rows(0)
    send_back(range(1, 4))
    gxb[pl.ds(0, cap), :] = gxs[pl.ds(0, cap), :]

    wait_half(SEND_X, 1, blk, xe)
    forward(1)
    xet[...] = jnp.transpose(xe[...])
    wait_half(SEND_MSG, 1, row, msg_r)
    wait_half(SEND_R, 1, blk, re)
    cotangents(1)
    send_dots(1)
    send_back(range(4, HALF))
    slot_grads(1)

    totals = tree_sum([msg_r[p] for p in range(DEVS)])
    spread = jnp.broadcast_to(totals, (DEVS, LANES))
    count_all = jnp.sum(where(lane == sub + cap, spread), axis=1, keepdims=True)
    prob_all = jnp.sum(where(lane == sub + cap + DEVS, spread), axis=1, keepdims=True)
    frac = count_all * (1.0 / tokens_all)
    for c in range(2):
        wait_half(SEND_DOT, c, row, dot_r)
    dots = rows_of(dot_r, range(DEVS), LANES)
    high, mid, low = split3(dots)
    hit1, hit2 = block1 == expert, block2 == expert
    find = lambda part, at, hit: jnp.sum(where(hit, dot(part, at)), axis=0, keepdims=True)
    grad1, grad2 = find(high, at1, hit1), find(high, at2, hit2)
    moe = norm1 * (grad1 + find(mid, at1, hit1) + find(low, at1, hit1))
    moe += norm2 * (grad2 + find(mid, at2, hit2) + find(low, at2, hit2))
    inv_sq = 1.0 / (gate_sum * gate_sum)
    dgate1 = (grad1 - grad2) * gate2 * inv_sq
    dgate2 = (grad2 - grad1) * gate1 * inv_sq
    dprob = dgate1 * hot1 + dgate2 * hot2 + (ALPHA * hidden * DEVS) * frac
    dlogits = prob * (dprob - jnp.sum(prob * dprob, axis=0, keepdims=True))
    grad_gate = dot(dlogits.astype(BF16), x[...])
    part = jnp.broadcast_to(own + jnp.sum(moe, axis=1, keepdims=True), (DEVS, LANES))
    reduced = jnp.concatenate([grad_gate, part], axis=1)
    for e in range(DEVS):
        red_s[e] = reduced[e:e + 1]
    red_r[0] = red_s[me]
    back_rows(1)
    for p in others:
        remote(SEND_RS, p, red_s.at[pl.ds(peer(p), 1)], row(red_r, p)).start()
    send_back(halves[1])

    @pl.loop(0, tiles, unroll=2)
    def _(n):
        cols = pl.ds(pl.multiple_of(n * wide, wide), wide)
        dw2_ref[cols, :] = dot(actt[cols, :], gy[...]).astype(BF16)

    for c in range(2):
        wait_half(SEND_RS, c, row, red_r)
    total = tree_sum([red_r[p] for p in range(DEVS)])
    row_s[0] = total[:, :hidden]
    row_r[0] = total[:, :hidden]
    for p in others:
        remote(SEND_AG, p, row(row_s, 0), row(row_r, p)).start()
    aux = DEVS * jnp.sum(frac * (prob_all * (1.0 / tokens_all)), axis=0, keepdims=True)
    loss = total[:, hidden:hidden + 1] * (1.0 / numel) + ALPHA * aux
    loss_ref[...] = jnp.broadcast_to(loss, loss_ref.shape)

    @pl.loop(0, tiles, unroll=2)
    def _(n):
        cols = pl.ds(pl.multiple_of(n * wide, wide), wide)
        dw1_ref[:, cols] = dot(xet[...], dpre[:, cols]).astype(BF16)

    dlog_pad = jnp.concatenate([dlogits, jnp.zeros((LANES - DEVS, seq), F32)], axis=0)
    gate_pad = jnp.concatenate([wg[...], jnp.zeros((LANES - DEVS, hidden), BF16)], axis=0)
    router = dot(jnp.transpose(dlog_pad).astype(BF16), gate_pad)
    acc[...] = r[...].astype(F32) + router
    for c in range(2):
        wait_half(SEND_GX, c, blk, gxb)
    gx_ref[...] = (acc[...] + dot(dispt[...], gxb[...])).astype(BF16)
    for c in range(2):
        wait_half(SEND_AG, c, row, row_r)
    gw_ref[...] = rows_of(row_r, [peer(p) for p in range(DEVS)], hidden)

    for kind, view in ((SEND_X, blk(xs, 1, 15)), (SEND_R, blk(rs, 1, 15)), (SEND_GX, blk(gxs, 1, 15)),
                       (SEND_MSG, row(msg_s, 1, 15)), (SEND_DOT, row(dot_s, 1, 15)),
                       (SEND_RS, row(red_s, 1, 15)), (SEND_AG, row(row_r, 1, 15))):
        remote(kind, 1, view, view).wait_send()


def store_kernel(loss, gx, dw1, dw2, gw, loss_out, gx_out, dw1_out, dw2_out, gw_out, sem):
    pairs = [(gx, gx_out), (gw, gw_out)]
    for big, out in ((dw1, dw1_out), (dw2, dw2_out)):
        step = big.shape[0] // 4
        pairs += [(big.at[pl.ds(i * step, step)], out.at[pl.ds(i * step, step)]) for i in range(4)]
    copies = [pltpu.make_async_copy(src, dst, sem.at[i]) for i, (src, dst) in enumerate(pairs)]
    for copy in copies:
        copy.start()
    loss_out[0, 0] = jnp.max(loss[...])
    for copy in copies:
        copy.wait()


def solution(mesh):
    def layer_body(x_loc, r_loc, w_gate, w_in_loc, w_out_loc, first_ids, second_ids, keep_ids):
        _, seq, hidden = x_loc.shape
        ff = w_in_loc.shape[2]
        cap = 2 * seq // DEVS
        slots = DEVS * cap
        anyspace = pl.BlockSpec(memory_space=pl.ANY)
        vmem = pl.BlockSpec(memory_space=pltpu.VMEM)
        results = pl.pallas_call(
            functools.partial(layer_kernel, cap),
            out_shape=(
                pltpu.VMEM((8, LANES), F32),
                pltpu.VMEM((seq, hidden), BF16),
                pltpu.VMEM((hidden, ff), BF16),
                pltpu.VMEM((ff, hidden), BF16),
                pltpu.VMEM((DEVS, hidden), F32),
            ),
            in_specs=[anyspace] * 8,
            out_specs=(vmem,) * 5,
            scratch_shapes=[
                pltpu.VMEM((seq, hidden), BF16),
                pltpu.VMEM((seq, hidden), BF16),
                pltpu.VMEM((DEVS, hidden), BF16),
                pltpu.VMEM((hidden, ff), BF16),
                pltpu.VMEM((ff, hidden), BF16),
                pltpu.VMEM((3 + PAD, 1, seq), jnp.int32),
                pltpu.VMEM((slots, seq), BF16),
                pltpu.VMEM((seq, slots), BF16),
                pltpu.VMEM((slots, hidden), BF16),
                pltpu.VMEM((slots, hidden), BF16),
                pltpu.VMEM((slots, hidden), BF16),
                pltpu.VMEM((slots, hidden), BF16),
                pltpu.VMEM((slots, hidden), BF16),
                pltpu.VMEM((2, HALF * cap, 512), F32),
                pltpu.VMEM((slots, ff), BF16),
                pltpu.VMEM((ff, slots), BF16),
                pltpu.VMEM((HALF * cap, hidden), F32),
                pltpu.VMEM((slots, ff), F32),
                pltpu.VMEM((slots, ff), BF16),
                pltpu.VMEM((slots, hidden), BF16),
                pltpu.VMEM((slots, hidden), BF16),
                pltpu.VMEM((slots, hidden), BF16),
                pltpu.VMEM((hidden, slots), BF16),
                pltpu.VMEM((DEVS + PAD, 1, LANES), F32),
                pltpu.VMEM((DEVS + PAD, 1, LANES), F32),
                pltpu.VMEM((DEVS + PAD, 1, LANES), F32),
                pltpu.VMEM((DEVS + PAD, 1, LANES), F32),
                pltpu.VMEM((DEVS + PAD, 1, hidden + LANES), F32),
                pltpu.VMEM((DEVS + PAD, 1, hidden + LANES), F32),
                pltpu.VMEM((1 + PAD, 1, hidden), F32),
                pltpu.VMEM((DEVS + PAD, 1, hidden), F32),
                pltpu.SemaphoreType.DMA((6,)),
                pltpu.SemaphoreType.DMA((7,)),
                pltpu.SemaphoreType.DMA((7, 2)),
            ],
            compiler_params=pltpu.CompilerParams(
                collective_id=0, has_side_effects=True, vmem_limit_bytes=48 * 1024 * 1024),
            name="moe_layer",
        )(x_loc[0], r_loc[0], w_gate.T, w_in_loc[0], w_out_loc[0], first_ids, second_ids, keep_ids)
        loss, gx, dw1, dw2, gw = pl.pallas_call(
            store_kernel,
            out_shape=(
                jax.ShapeDtypeStruct((1, 1), F32),
                jax.ShapeDtypeStruct((seq, hidden), BF16),
                jax.ShapeDtypeStruct((hidden, ff), BF16),
                jax.ShapeDtypeStruct((ff, hidden), BF16),
                jax.ShapeDtypeStruct((DEVS, hidden), F32),
            ),
            in_specs=[vmem] * 5,
            out_specs=(pl.BlockSpec(memory_space=pltpu.SMEM),) + (anyspace,) * 4,
            scratch_shapes=[pltpu.SemaphoreType.DMA((10,))],
            compiler_params=pltpu.CompilerParams(vmem_limit_bytes=2 * 1024 * 1024),
            name="store_results",
        )(*results)
        return loss.reshape(()), gx[None], dw1[None], dw2[None], gw.T

    row_spec = P('ep', None, None)
    id_spec = P('ep', None)
    return jax.shard_map(layer_body, mesh=mesh, in_specs=(row_spec, row_spec, P(None, None), row_spec, row_spec, id_spec, id_spec, id_spec), out_specs=(P(), row_spec, row_spec, row_spec, P(None, None)), check_vma=False)
```

```python
import functools

import jax
import jax.numpy as jnp
from jax import lax
from jax.experimental import pallas as pl
from jax.experimental.pallas import tpu as pltpu
from jax.sharding import PartitionSpec as P

ALPHA = 0.01
MESH = pl.DeviceIdType.MESH
F32 = jnp.float32
BF16 = jnp.bfloat16

DEVS = 16
LANES = 128
PAD = 8
HALF = 8

SEND_X, SEND_R, SEND_MSG, SEND_DOT, SEND_GX, SEND_RS, SEND_AG = range(7)


def offset_of(p):
    x, y = (p >> 1) & 1, (p >> 2) & 1
    z = x ^ y ^ ((p >> 3) & 1)
    return (p & 1) | (x << 1) | (y << 2) | (z << 3)


def block_of(ids, me):
    k = jnp.bitwise_xor(ids, me)
    parity = (k >> 1) ^ (k >> 2) ^ (k >> 3)
    return (k & 7) + 8 * (parity & 1)


def dot(a, b, ca=1, cb=0):
    return lax.dot_general(a, b, (((ca,), (cb,)), ((), ())), preferred_element_type=F32)


def iota(shape, axis):
    return lax.broadcasted_iota(jnp.int32, shape, axis)


def where(mask, value):
    return jnp.where(mask, value, jnp.zeros_like(value))


def tree_sum(rows):
    rows = list(rows)
    while len(rows) > 1:
        rows = [rows[i] + rows[i + 1] for i in range(0, len(rows), 2)]
    return rows[0]


def rows_of(ref, places, width):
    n = len(places)
    out = jnp.zeros((n, width), F32)
    sub = iota((n, width), 0)
    for i, place in enumerate(places):
        out = jnp.where(sub == place, jnp.broadcast_to(ref[i], (n, width)), out)
    return out


def split3(values):
    high = values.astype(BF16)
    rest = values - high.astype(F32)
    mid = rest.astype(BF16)
    return high, mid, (rest - mid.astype(F32)).astype(BF16)


def layer_kernel(cap, x_hbm, r_hbm, wg_hbm, w1_hbm, w2_hbm, e1_hbm, e2_hbm, k2_hbm,
                 loss_ref, gw_ref, dw2_ref, dw1_ref, xet, dpre, dispt, gxb, base,
                 x, r, wg, w1, w2, w1t, w2t, ids, disp, xs, rs, xe, re, gy, pre, act, actt, acc, slope, ybuf, gxs,
                 msg_s, msg_r, dot_s, dot_r, red_s, red_r, row_s, row_r,
                 local_sem, send_sem, recv_sem):
    seq, hidden = x.shape
    ff = w1.shape[1]
    half = HALF * cap
    tokens_all = DEVS * seq
    numel = tokens_all * hidden

    me = lax.axis_index("ep")
    bits = [lax.rem(me // (1 << i), 2) for i in range(4)]

    def peer(p):
        k = offset_of(p)
        return sum(((1 - bits[i]) if (k >> i) & 1 else bits[i]) * (1 << i) for i in range(4))

    def remote(kind, p, src, dst):
        return pltpu.make_async_remote_copy(
            src_ref=src, dst_ref=dst, send_sem=send_sem.at[kind], recv_sem=recv_sem.at[kind, p // HALF],
            device_id=(peer(p),), device_id_type=MESH)

    others = range(1, DEVS)
    halves = (range(1, HALF), range(HALF, DEVS))
    orders = ((2, 4, 6, 3, 5, 7, 1), (14, 15, 8, 10, 12, 9, 11, 13))
    blk = lambda ref, p, n=1: ref.at[pl.ds(p * cap, n * cap), :]
    row = lambda ref, p, n=1: ref.at[pl.ds(p, n)]

    def wait_half(kind, c, part, ref):
        first, count = halves[c][0], len(halves[c])
        view = part(ref, first, count)
        remote(kind, first, view, view).wait_recv()

    id_copies = [pltpu.make_async_copy(src, ids.at[i], local_sem.at[0]) for i, src in enumerate((e1_hbm, e2_hbm, k2_hbm))]
    id_wait = pltpu.make_async_copy(row(ids, 0, 3), row(ids, 0, 3), local_sem.at[0])
    x_copy, r_copy, wg_copy, w1_copy, w2_copy = [
        pltpu.make_async_copy(src, dst, local_sem.at[1 + i]) for i, (src, dst) in enumerate((
            (x_hbm, x), (r_hbm, r), (wg_hbm, wg), (w1_hbm, w1), (w2_hbm, w2)))]
    barrier = pltpu.get_barrier_semaphore()
    for p in others:
        pl.semaphore_signal(barrier, inc=1, device_id=(peer(p),), device_id_type=MESH)
    for copy in id_copies + [x_copy, r_copy, wg_copy, w1_copy, w2_copy]:
        copy.start()

    expert = iota((DEVS, seq), 0)
    earlier = (iota((seq, seq), 0) < iota((seq, seq), 1)).astype(F32).astype(BF16)
    id_wait.wait()
    e1, e2, k2 = ids[0], ids[1], ids[2]
    hot1 = (e1 == expert).astype(F32)
    hot2 = (e2 == expert).astype(F32)
    kept2 = hot2 * k2.astype(F32)
    before = dot(jnp.concatenate([hot1, kept2], axis=0).astype(BF16), earlier)
    count1 = jnp.sum(hot1, axis=1, keepdims=True)
    pos1 = jnp.sum(before[:DEVS] * hot1, axis=0, keepdims=True).astype(jnp.int32)
    pos2 = jnp.sum((before[DEVS:] + count1) * hot2, axis=0, keepdims=True).astype(jnp.int32)
    keep1 = pos1 < cap
    keep2 = (pos2 < cap) & (k2 > 0)
    block1, block2 = block_of(e1, me), block_of(e2, me)
    slot1 = jnp.where(keep1, block1 * cap + pos1, -1)
    slot2 = jnp.where(keep2, block2 * cap + pos2, -1)

    half_rows = [pl.ds(c * half, half) for c in range(2)]

    def dispatch_x(c):
        slot = iota((half, seq), 0) + c * half
        table = ((slot == slot1) | (slot == slot2)).astype(F32).astype(BF16)
        disp[half_rows[c], :] = table
        xs[half_rows[c], :] = dot(table, x[...]).astype(BF16)

    def dispatch_r(c):
        rs[half_rows[c], :] = dot(disp[half_rows[c], :], r[...]).astype(BF16)

    def send_blocks(kind, c, src, dst):
        for p in orders[c]:
            remote(kind, p, blk(src, p), blk(dst, p)).start()

    x_copy.wait()
    dispatch_x(0)
    pl.semaphore_wait(barrier, DEVS - 1)
    send_blocks(SEND_X, 0, xs, xe)
    xe[pl.ds(0, cap), :] = xs[pl.ds(0, cap), :]
    r_copy.wait()
    dispatch_r(0)
    wg_copy.wait()
    logits = dot(wg[...], x[...], 1, 1)
    shifted = jnp.exp(logits - jnp.max(logits, axis=0, keepdims=True))
    prob = shifted / jnp.sum(shifted, axis=0, keepdims=True)
    gate1 = jnp.sum(prob * hot1, axis=0, keepdims=True)
    gate2 = jnp.sum(prob * hot2, axis=0, keepdims=True)
    gate_sum = gate1 + gate2
    norm1 = (gate1 / gate_sum).astype(BF16).astype(F32)
    norm2 = (gate2 / gate_sum).astype(BF16).astype(F32)
    place = iota((LANES, seq), 0)
    at1 = (place == jnp.where(keep1, pos1, -1)).astype(F32).astype(BF16)
    at2 = (place == jnp.where(keep2, pos2, -1)).astype(F32).astype(BF16)
    weights = dot((hot1 * norm1).astype(BF16), at1, 1, 1) + dot((hot2 * norm2).astype(BF16), at2, 1, 1)
    prob_sum = jnp.sum(prob, axis=1, keepdims=True)
    sub, lane = iota((DEVS, LANES), 0), iota((DEVS, LANES), 1)
    stats = where(lane == sub + cap, jnp.broadcast_to(count1, (DEVS, LANES)))
    stats += where(lane == sub + cap + DEVS, jnp.broadcast_to(prob_sum, (DEVS, LANES)))
    message = weights + jnp.sum(stats, axis=0, keepdims=True)
    for e in range(DEVS):
        msg_s[e] = message[e:e + 1]
    msg_r[0] = msg_s[me]
    for p in orders[1] + orders[0]:
        remote(SEND_MSG, p, msg_s.at[pl.ds(peer(p), 1)], row(msg_r, p)).start()
    send_blocks(SEND_R, 0, rs, re)
    re[pl.ds(0, cap), :] = rs[pl.ds(0, cap), :]
    dispatch_x(1)
    dispatch_r(1)
    send_blocks(SEND_X, 1, xs, xe)
    send_blocks(SEND_R, 1, rs, re)
    dispt[...] = jnp.transpose(disp[...])
    own = jnp.sum(jnp.sum(x[...].astype(F32) * r[...].astype(F32), axis=0, keepdims=True), axis=1, keepdims=True)

    wide = 512
    tiles = ff // wide
    tile = lambda n: pl.ds(n * wide, wide)
    diag = iota((half, LANES), 1) == lax.rem(iota((half, LANES), 0), cap)

    def forward(c):
        rows = half_rows[c]
        for n in range(tiles + 2):
            if n < tiles:
                pre[n % 2] = dot(xe[rows, :], w1[:, tile(n)])
            if 1 <= n <= tiles:
                m = n - 1
                v = pre[m % 2]
                sq = v * v
                root = 0.7978845608028654
                t = jnp.tanh(v * (root + root * 0.044715 * sq))
                hx = 0.5 * v
                a = (hx + hx * t).astype(BF16)
                act[rows, tile(m)] = a
                actt[tile(m), rows] = jnp.transpose(a)
                slope[rows, tile(m)] = (0.5 + 0.5 * t) + hx * (1.0 - t * t) * (root + 3.0 * root * 0.044715 * sq)
            if n >= 2:
                m = n - 2
                y = dot(act[rows, tile(m)], w2[tile(m), :])
                if m:
                    y += acc[...]
                if m < tiles - 1:
                    acc[...] = y
                else:
                    ybuf[rows, :] = y.astype(BF16)

    def cotangents(c):
        rows = half_rows[c]
        mine = range(c * HALF, (c + 1) * HALF)
        spread = jnp.concatenate([jnp.broadcast_to(msg_r[p], (cap, LANES)) for p in mine], axis=0)
        weight = jnp.sum(where(diag, spread), axis=1, keepdims=True)
        r_rows = re[rows, :].astype(F32)
        gy[rows, :] = (r_rows * weight).astype(BF16)
        dots = jnp.sum(r_rows * ybuf[rows, :].astype(F32), axis=1, keepdims=True)
        dot_mat = where(diag, jnp.broadcast_to(dots, (half, LANES)))
        for p in mine:
            q = (p - c * HALF) * cap
            (dot_s if p else dot_r)[p] = jnp.sum(dot_mat[q:q + cap], axis=0, keepdims=True)

    def slot_grads(first, count):
        rows = pl.ds(first * cap, count * cap)
        for n in range(tiles):
            da = dot(gy[rows, :], w2t[:, tile(n)]).astype(BF16).astype(F32)
            dpre[rows, tile(n)] = (da * slope[rows, tile(n)]).astype(BF16)
        gxs[rows, :] = dot(dpre[rows, :], w1t[...]).astype(BF16)

    def send_dots(c):
        for p in orders[c]:
            remote(SEND_DOT, p, row(dot_s, p), row(dot_r, p)).start()

    def send_back(blocks):
        for p in blocks:
            remote(SEND_GX, p, blk(gxs, p), blk(gxb, p)).start()

    w1_copy.wait()
    w2_copy.wait()

    @pl.loop(0, tiles)
    def _(n):
        cols = pl.ds(pl.multiple_of(n * wide, wide), wide)
        w2t[:, cols] = jnp.transpose(w2[cols, :])
        w1t[cols, :] = jnp.transpose(w1[:, cols])

    wait_half(SEND_X, 0, blk, xe)
    forward(0)
    wait_half(SEND_MSG, 0, row, msg_r)
    wait_half(SEND_R, 0, blk, re)
    cotangents(0)
    send_dots(0)
    slot_grads(0, HALF)
    send_back((2, 4, 1))
    gxb[pl.ds(0, cap), :] = gxs[pl.ds(0, cap), :]

    wait_half(SEND_X, 1, blk, xe)
    forward(1)
    xet[...] = jnp.transpose(xe[...])
    wait_half(SEND_MSG, 1, row, msg_r)
    wait_half(SEND_R, 1, blk, re)
    cotangents(1)
    send_dots(1)
    send_back((6, 3, 5, 7))
    slot_grads(12, 4)
    send_back((14, 15, 12, 13))
    slot_grads(8, 4)

    totals = tree_sum([msg_r[p] for p in range(DEVS)])
    spread = jnp.broadcast_to(totals, (DEVS, LANES))
    count_all = jnp.sum(where(lane == sub + cap, spread), axis=1, keepdims=True)
    prob_all = jnp.sum(where(lane == sub + cap + DEVS, spread), axis=1, keepdims=True)
    frac = count_all * (1.0 / tokens_all)
    for c in range(2):
        wait_half(SEND_DOT, c, row, dot_r)
    dots = rows_of(dot_r, range(DEVS), LANES)
    high, mid, low = split3(dots)
    hit1, hit2 = block1 == expert, block2 == expert
    find = lambda part, at, hit: jnp.sum(where(hit, dot(part, at)), axis=0, keepdims=True)
    grad1, grad2 = find(high, at1, hit1), find(high, at2, hit2)
    moe = norm1 * (grad1 + find(mid, at1, hit1) + find(low, at1, hit1))
    moe += norm2 * (grad2 + find(mid, at2, hit2) + find(low, at2, hit2))
    inv_sq = 1.0 / (gate_sum * gate_sum)
    dgate1 = (grad1 - grad2) * gate2 * inv_sq
    dgate2 = (grad2 - grad1) * gate1 * inv_sq
    dprob = dgate1 * hot1 + dgate2 * hot2 + (ALPHA * hidden * DEVS) * frac
    dlogits = prob * (dprob - jnp.sum(prob * dprob, axis=0, keepdims=True))
    grad_gate = dot(dlogits.astype(BF16), x[...])
    part = jnp.broadcast_to(own + jnp.sum(moe, axis=1, keepdims=True), (DEVS, LANES))
    reduced = jnp.concatenate([grad_gate, part], axis=1)
    for e in range(DEVS):
        red_s[e] = reduced[e:e + 1]
    red_r[0] = red_s[me]
    for p in orders[1] + orders[0]:
        remote(SEND_RS, p, red_s.at[pl.ds(peer(p), 1)], row(red_r, p)).start()
    send_back((8, 10, 9, 11))

    @pl.loop(0, tiles, unroll=2)
    def _(n):
        cols = pl.ds(pl.multiple_of(n * wide, wide), wide)
        dw2_ref[cols, :] = dot(actt[cols, :], gy[...]).astype(BF16)

    for c in range(2):
        wait_half(SEND_RS, c, row, red_r)
    total = tree_sum([red_r[p] for p in range(DEVS)])
    row_s[0] = total[:, :hidden]
    row_r[0] = total[:, :hidden]
    for p in orders[1] + orders[0]:
        remote(SEND_AG, p, row(row_s, 0), row(row_r, p)).start()
    aux = DEVS * jnp.sum(frac * (prob_all * (1.0 / tokens_all)), axis=0, keepdims=True)
    loss = total[:, hidden:hidden + 1] * (1.0 / numel) + ALPHA * aux
    loss_ref[...] = jnp.broadcast_to(loss, loss_ref.shape)

    @pl.loop(0, dw1_ref.shape[0])
    def _(n):
        dw1_ref[n] = dot(xet[...], dpre[:, pl.ds(pl.multiple_of(n * wide, wide), wide)]).astype(BF16)

    dlog_pad = jnp.concatenate([dlogits, jnp.zeros((LANES - DEVS, seq), F32)], axis=0)
    gate_pad = jnp.concatenate([wg[...], jnp.zeros((LANES - DEVS, hidden), BF16)], axis=0)
    base[...] = r[...].astype(F32) + dot(jnp.transpose(dlog_pad).astype(BF16), gate_pad)
    for c in range(2):
        wait_half(SEND_GX, c, blk, gxb)
    for c in range(2):
        wait_half(SEND_AG, c, row, row_r)
    gw_ref[...] = rows_of(row_r, [peer(p) for p in range(DEVS)], hidden)

    for kind, view in ((SEND_X, blk(xs, 1, 15)), (SEND_R, blk(rs, 1, 15)), (SEND_GX, blk(gxs, 1, 15)),
                       (SEND_MSG, row(msg_s, 1, 15)), (SEND_DOT, row(dot_s, 1, 15)),
                       (SEND_RS, row(red_s, 1, 15)), (SEND_AG, row(row_r, 1, 15))):
        remote(kind, 1, view, view).wait_send()


def store_kernel(loss, gw, dw2, dw1, xet, dpre, dispt, gxb, base,
                 loss_out, gx_out, dw1_out, dw2_out, gw_out, gx, tiles, sem):
    done, _, wide = dw1.shape
    more = tiles.shape[0]
    tile = lambda n: pl.ds(n * wide, wide)
    pairs = [(dw2, dw2_out), (gw, gw_out)] + [(dw1.at[n], dw1_out.at[:, tile(n)]) for n in range(done)]
    pairs += [(tiles.at[n], dw1_out.at[:, tile(done + n)]) for n in range(more)] + [(gx, gx_out)]
    copies = [pltpu.make_async_copy(src, dst, sem.at[i]) for i, (src, dst) in enumerate(pairs)]
    for copy in copies[:2 + done]:
        copy.start()
    for n in range(more):
        tiles[n] = dot(xet[...], dpre[:, tile(done + n)]).astype(BF16)
        copies[2 + done + n].start()
    gx[...] = (base[...] + dot(dispt[...], gxb[...])).astype(BF16)
    copies[-1].start()
    loss_out[0, 0] = jnp.max(loss[...])
    for copy in copies:
        copy.wait()


def solution(mesh):
    def layer_body(x_loc, r_loc, w_gate, w_in_loc, w_out_loc, first_ids, second_ids, keep_ids):
        _, seq, hidden = x_loc.shape
        ff = w_in_loc.shape[2]
        cap = 2 * seq // DEVS
        slots = DEVS * cap
        anyspace = pl.BlockSpec(memory_space=pl.ANY)
        vmem = pl.BlockSpec(memory_space=pltpu.VMEM)
        wide, early = 512, 4
        late = ff // wide - early
        results = pl.pallas_call(
            functools.partial(layer_kernel, cap),
            out_shape=(
                pltpu.VMEM((8, LANES), F32),
                pltpu.VMEM((DEVS, hidden), F32),
                pltpu.VMEM((ff, hidden), BF16),
                pltpu.VMEM((early, hidden, wide), BF16),
                pltpu.VMEM((hidden, slots), BF16),
                pltpu.VMEM((slots, ff), BF16),
                pltpu.VMEM((seq, slots), BF16),
                pltpu.VMEM((slots, hidden), BF16),
                pltpu.VMEM((seq, hidden), F32),
            ),
            in_specs=[anyspace] * 8,
            out_specs=(vmem,) * 9,
            scratch_shapes=[
                pltpu.VMEM((seq, hidden), BF16),
                pltpu.VMEM((seq, hidden), BF16),
                pltpu.VMEM((DEVS, hidden), BF16),
                pltpu.VMEM((hidden, ff), BF16),
                pltpu.VMEM((ff, hidden), BF16),
                pltpu.VMEM((ff, hidden), BF16),
                pltpu.VMEM((hidden, ff), BF16),
                pltpu.VMEM((3 + PAD, 1, seq), jnp.int32),
                pltpu.VMEM((slots, seq), BF16),
                pltpu.VMEM((slots, hidden), BF16),
                pltpu.VMEM((slots, hidden), BF16),
                pltpu.VMEM((slots, hidden), BF16),
                pltpu.VMEM((slots, hidden), BF16),
                pltpu.VMEM((slots, hidden), BF16),
                pltpu.VMEM((2, HALF * cap, 512), F32),
                pltpu.VMEM((slots, ff), BF16),
                pltpu.VMEM((ff, slots), BF16),
                pltpu.VMEM((HALF * cap, hidden), F32),
                pltpu.VMEM((slots, ff), F32),
                pltpu.VMEM((slots, hidden), BF16),
                pltpu.VMEM((slots, hidden), BF16),
                pltpu.VMEM((DEVS + PAD, 1, LANES), F32),
                pltpu.VMEM((DEVS + PAD, 1, LANES), F32),
                pltpu.VMEM((DEVS + PAD, 1, LANES), F32),
                pltpu.VMEM((DEVS + PAD, 1, LANES), F32),
                pltpu.VMEM((DEVS + PAD, 1, hidden + LANES), F32),
                pltpu.VMEM((DEVS + PAD, 1, hidden + LANES), F32),
                pltpu.VMEM((1 + PAD, 1, hidden), F32),
                pltpu.VMEM((DEVS + PAD, 1, hidden), F32),
                pltpu.SemaphoreType.DMA((6,)),
                pltpu.SemaphoreType.DMA((7,)),
                pltpu.SemaphoreType.DMA((7, 2)),
            ],
            compiler_params=pltpu.CompilerParams(
                collective_id=0, has_side_effects=True, vmem_limit_bytes=48 * 1024 * 1024),
            name="moe_layer",
        )(x_loc[0], r_loc[0], w_gate.T, w_in_loc[0], w_out_loc[0], first_ids, second_ids, keep_ids)
        loss, gx, dw1, dw2, gw = pl.pallas_call(
            store_kernel,
            out_shape=(
                jax.ShapeDtypeStruct((1, 1), F32),
                jax.ShapeDtypeStruct((seq, hidden), BF16),
                jax.ShapeDtypeStruct((hidden, ff), BF16),
                jax.ShapeDtypeStruct((ff, hidden), BF16),
                jax.ShapeDtypeStruct((DEVS, hidden), F32),
            ),
            in_specs=[vmem] * 9,
            out_specs=(pl.BlockSpec(memory_space=pltpu.SMEM),) + (anyspace,) * 4,
            scratch_shapes=[
                pltpu.VMEM((seq, hidden), BF16),
                pltpu.VMEM((late, hidden, wide), BF16),
                pltpu.SemaphoreType.DMA((3 + ff // wide,)),
            ],
            compiler_params=pltpu.CompilerParams(vmem_limit_bytes=12 * 1024 * 1024),
            name="store_results",
        )(*results)
        return loss.reshape(()), gx[None], dw1[None], dw2[None], gw.T

    row_spec = P('ep', None, None)
    id_spec = P('ep', None)
    return jax.shard_map(layer_body, mesh=mesh, in_specs=(row_spec, row_spec, P(None, None), row_spec, row_spec, id_spec, id_spec, id_spec), out_specs=(P(), row_spec, row_spec, row_spec, P(None, None)), check_vma=False)
```

```python
import functools

import jax
import jax.numpy as jnp
from jax import lax
from jax.experimental import pallas as pl
from jax.experimental.pallas import tpu as pltpu
from jax.sharding import PartitionSpec as P

ALPHA = 0.01
MESH = pl.DeviceIdType.MESH
F32 = jnp.float32
BF16 = jnp.bfloat16

DEVS = 16
LANES = 128
PAD = 8
HALF = 8

SEND_X, SEND_R, SEND_MSG, SEND_DOT, SEND_GX, SEND_RS, SEND_AG = range(7)


def offset_of(p):
    x, y, core = p & 1, (p >> 1) & 1, (p >> 2) & 1
    z = x ^ y ^ (p >> 3)
    return core | (x << 1) | (y << 2) | (z << 3)


def block_of(ids, me):
    k = jnp.bitwise_xor(ids, me)
    core, x, y, z = [(k >> i) & 1 for i in range(4)]
    return x + 2 * y + 4 * core + 8 * (x ^ y ^ z)


def dot(a, b, ca=1, cb=0):
    return lax.dot_general(a, b, (((ca,), (cb,)), ((), ())), preferred_element_type=F32)


def iota(shape, axis):
    return lax.broadcasted_iota(jnp.int32, shape, axis)


def where(mask, value):
    return jnp.where(mask, value, jnp.zeros_like(value))


def tree_sum(rows):
    rows = list(rows)
    while len(rows) > 1:
        rows = [rows[i] + rows[i + 1] for i in range(0, len(rows), 2)]
    return rows[0]


def rows_of(ref, places, width):
    n = len(places)
    out = jnp.zeros((n, width), F32)
    sub = iota((n, width), 0)
    for i, place in enumerate(places):
        out = jnp.where(sub == place, jnp.broadcast_to(ref[i], (n, width)), out)
    return out


def split3(values):
    high = values.astype(BF16)
    rest = values - high.astype(F32)
    mid = rest.astype(BF16)
    return high, mid, (rest - mid.astype(F32)).astype(BF16)


def layer_kernel(cap, x_hbm, r_hbm, wg_hbm, w1_hbm, w2_hbm, e1_hbm, e2_hbm, k2_hbm,
                 loss_ref, gw_ref, dw2_ref, dw1_ref, xet, dpre, dispt, gxb, base,
                 x, r, wg, w1, w2, w1t, w2t, ids, disp, xs, rs, xe, re, gy, pre, act, actt, acc, slope, ybuf, gxs,
                 msg_s, msg_r, dot_s, dot_r, red_s, red_r, row_s, row_r,
                 local_sem, send_sem, recv_sem):
    seq, hidden = x.shape
    ff = w1.shape[1]
    half = HALF * cap
    tokens_all = DEVS * seq
    numel = tokens_all * hidden

    me = lax.axis_index("ep")
    bits = [lax.rem(me // (1 << i), 2) for i in range(4)]

    def peer(p):
        k = offset_of(p)
        return sum(((1 - bits[i]) if (k >> i) & 1 else bits[i]) * (1 << i) for i in range(4))

    def remote(kind, p, src, dst):
        return pltpu.make_async_remote_copy(
            src_ref=src, dst_ref=dst, send_sem=send_sem.at[kind], recv_sem=recv_sem.at[kind, p // HALF],
            device_id=(peer(p),), device_id_type=MESH)

    others = range(1, DEVS)
    halves = (range(1, HALF), range(HALF, DEVS))
    orders = ((1, 2, 3, 5, 6, 7, 4), (11, 15, 8, 9, 10, 12, 13, 14))
    blk = lambda ref, p, n=1: ref.at[pl.ds(p * cap, n * cap), :]
    row = lambda ref, p, n=1: ref.at[pl.ds(p, n)]

    def wait_half(kind, c, part, ref):
        first, count = halves[c][0], len(halves[c])
        view = part(ref, first, count)
        remote(kind, first, view, view).wait_recv()

    id_copies = [pltpu.make_async_copy(src, ids.at[i], local_sem.at[0]) for i, src in enumerate((e1_hbm, e2_hbm, k2_hbm))]
    id_wait = pltpu.make_async_copy(row(ids, 0, 3), row(ids, 0, 3), local_sem.at[0])
    x_copy, r_copy, wg_copy, w1_copy, w2_copy = [
        pltpu.make_async_copy(src, dst, local_sem.at[1 + i]) for i, (src, dst) in enumerate((
            (x_hbm, x), (r_hbm, r), (wg_hbm, wg), (w1_hbm, w1), (w2_hbm, w2)))]
    barrier = pltpu.get_barrier_semaphore()
    for p in others:
        pl.semaphore_signal(barrier, inc=1, device_id=(peer(p),), device_id_type=MESH)
    for copy in id_copies + [x_copy, r_copy, wg_copy, w1_copy, w2_copy]:
        copy.start()

    expert = iota((DEVS, seq), 0)
    earlier = (iota((seq, seq), 0) < iota((seq, seq), 1)).astype(F32).astype(BF16)
    id_wait.wait()
    e1, e2, k2 = ids[0], ids[1], ids[2]
    hot1 = (e1 == expert).astype(F32)
    hot2 = (e2 == expert).astype(F32)
    kept2 = hot2 * k2.astype(F32)
    before = dot(jnp.concatenate([hot1, kept2], axis=0).astype(BF16), earlier)
    count1 = jnp.sum(hot1, axis=1, keepdims=True)
    pos1 = jnp.sum(before[:DEVS] * hot1, axis=0, keepdims=True).astype(jnp.int32)
    pos2 = jnp.sum((before[DEVS:] + count1) * hot2, axis=0, keepdims=True).astype(jnp.int32)
    keep1 = pos1 < cap
    keep2 = (pos2 < cap) & (k2 > 0)
    block1, block2 = block_of(e1, me), block_of(e2, me)
    slot1 = jnp.where(keep1, block1 * cap + pos1, -1)
    slot2 = jnp.where(keep2, block2 * cap + pos2, -1)

    half_rows = [pl.ds(c * half, half) for c in range(2)]

    def dispatch_x(c):
        slot = iota((half, seq), 0) + c * half
        table = ((slot == slot1) | (slot == slot2)).astype(F32).astype(BF16)
        disp[half_rows[c], :] = table
        xs[half_rows[c], :] = dot(table, x[...]).astype(BF16)

    def dispatch_r(c):
        rs[half_rows[c], :] = dot(disp[half_rows[c], :], r[...]).astype(BF16)

    def send_blocks(kind, c, src, dst):
        for p in orders[c]:
            remote(kind, p, blk(src, p), blk(dst, p)).start()

    x_copy.wait()
    dispatch_x(0)
    pl.semaphore_wait(barrier, DEVS - 1)
    send_blocks(SEND_X, 0, xs, xe)
    xe[pl.ds(0, cap), :] = xs[pl.ds(0, cap), :]
    dispatch_x(1)
    send_blocks(SEND_X, 1, xs, xe)
    r_copy.wait()
    dispatch_r(0)
    wg_copy.wait()
    logits = dot(wg[...], x[...], 1, 1)
    shifted = jnp.exp(logits - jnp.max(logits, axis=0, keepdims=True))
    prob = shifted / jnp.sum(shifted, axis=0, keepdims=True)
    gate1 = jnp.sum(prob * hot1, axis=0, keepdims=True)
    gate2 = jnp.sum(prob * hot2, axis=0, keepdims=True)
    gate_sum = gate1 + gate2
    norm1, norm2 = gate1 / gate_sum, gate2 / gate_sum
    gamma = norm1 * norm2
    place = iota((LANES, seq), 0)

    def by_slot(first, second, shift):
        n = len(first)
        total = 0.0
        for hot, values, pos, keep in ((hot1, first, pos1, keep1), (hot2, second, pos2, keep2)):
            table = (place == jnp.where(keep, pos + shift, -1)).astype(F32).astype(BF16)
            stack = jnp.concatenate([hot * v.astype(F32) for v in values], axis=0).astype(BF16)
            total += dot(stack, table, 1, 1)
        return sum(total[i * DEVS:(i + 1) * DEVS] for i in range(n))

    gamma_parts = split3(gamma)
    message = by_slot([norm1.astype(BF16)], [norm2.astype(BF16)], 0)
    message += by_slot(gamma_parts, gamma_parts, cap) + by_slot([e2], [e1], 2 * cap)
    prob_sum = jnp.sum(prob, axis=1, keepdims=True)
    sub, lane = iota((DEVS, LANES), 0), iota((DEVS, LANES), 1)
    count_lane, prob_lane = lane == sub + 3 * cap, lane == sub + 3 * cap + DEVS
    stats = where(count_lane, jnp.broadcast_to(count1, (DEVS, LANES)))
    stats += where(prob_lane, jnp.broadcast_to(prob_sum, (DEVS, LANES)))
    message += jnp.sum(stats, axis=0, keepdims=True)
    for e in range(DEVS):
        msg_s[e] = message[e:e + 1]
    msg_r[0] = msg_s[me]
    for p in orders[1] + orders[0]:
        remote(SEND_MSG, p, msg_s.at[pl.ds(peer(p), 1)], row(msg_r, p)).start()
    send_blocks(SEND_R, 0, rs, re)
    re[pl.ds(0, cap), :] = rs[pl.ds(0, cap), :]
    dispatch_r(1)
    send_blocks(SEND_R, 1, rs, re)
    dispt[...] = jnp.transpose(disp[...])
    own = jnp.sum(jnp.sum(x[...].astype(F32) * r[...].astype(F32), axis=0, keepdims=True), axis=1, keepdims=True)

    wide = 512
    tiles = ff // wide
    tile = lambda n: pl.ds(n * wide, wide)
    lane_of, slot_of = iota((half, LANES), 1), lax.rem(iota((half, LANES), 0), cap)

    def forward(c):
        rows = half_rows[c]
        for n in range(tiles + 2):
            if n < tiles:
                pre[n % 2] = dot(xe[rows, :], w1[:, tile(n)])
            if 1 <= n <= tiles:
                m = n - 1
                v = pre[m % 2]
                sq = v * v
                root = 0.7978845608028654
                t = jnp.tanh(v * (root + root * 0.044715 * sq))
                hx = 0.5 * v
                a = (hx + hx * t).astype(BF16)
                act[rows, tile(m)] = a
                actt[tile(m), rows] = jnp.transpose(a)
                slope[rows, tile(m)] = (0.5 + 0.5 * t) + hx * (1.0 - t * t) * (root + 3.0 * root * 0.044715 * sq)
            if n >= 2:
                m = n - 2
                y = dot(act[rows, tile(m)], w2[tile(m), :])
                if m:
                    y += acc[...]
                if m < tiles - 1:
                    acc[...] = y
                else:
                    ybuf[rows, :] = y.astype(BF16)

    def cotangents(c):
        rows = half_rows[c]
        mine = range(c * HALF, (c + 1) * HALF)
        spread = jnp.concatenate([jnp.broadcast_to(msg_r[p], (cap, LANES)) for p in mine], axis=0)
        column = lambda i: jnp.sum(where(lane_of == slot_of + i * cap, spread), axis=1, keepdims=True)
        weight, scale, other = column(0), column(1), column(2)
        r_rows = re[rows, :].astype(F32)
        gy[rows, :] = (r_rows * weight).astype(BF16)
        dots = jnp.sum(r_rows * ybuf[rows, :].astype(F32), axis=1, keepdims=True)
        dot_mat = where(lane_of == slot_of, jnp.broadcast_to(dots, (half, LANES)))
        for p in mine:
            q = (p - c * HALF) * cap
            (dot_s if p else dot_r)[p] = jnp.sum(dot_mat[q:q + cap], axis=0, keepdims=True)
        share = jnp.broadcast_to(dots.astype(BF16).astype(F32) * scale, (half, LANES))
        table = where(lane_of == me, share) - where(lane_of == other.astype(jnp.int32), share)
        part = dot(jnp.transpose(table).astype(BF16), xe[rows, :])[:DEVS]
        return part, jnp.sum(weight * dots, axis=0, keepdims=True)

    def slot_grads(first, count):
        rows = pl.ds(first * cap, count * cap)
        for n in range(tiles):
            da = dot(gy[rows, :], w2t[:, tile(n)]).astype(BF16).astype(F32)
            dpre[rows, tile(n)] = (da * slope[rows, tile(n)]).astype(BF16)
        gxs[rows, :] = dot(dpre[rows, :], w1t[...]).astype(BF16)

    def send_dots(c):
        for p in orders[c]:
            remote(SEND_DOT, p, row(dot_s, p), row(dot_r, p)).start()

    def send_back(blocks):
        for p in blocks:
            remote(SEND_GX, p, blk(gxs, p), blk(gxb, p)).start()

    w1_copy.wait()
    w2_copy.wait()

    @pl.loop(0, tiles)
    def _(n):
        cols = pl.ds(pl.multiple_of(n * wide, wide), wide)
        w2t[:, cols] = jnp.transpose(w2[cols, :])
        w1t[cols, :] = jnp.transpose(w1[:, cols])

    for c in range(2):
        wait_half(SEND_X, c, blk, xe)
        forward(c)
    xet[...] = jnp.transpose(xe[...])

    for c in range(2):
        wait_half(SEND_MSG, c, row, msg_r)
    totals = jnp.broadcast_to(tree_sum([msg_r[p] for p in range(DEVS)]), (DEVS, LANES))
    frac = jnp.sum(where(count_lane, totals), axis=1, keepdims=True) * (1.0 / tokens_all)
    mean_prob = jnp.sum(where(prob_lane, totals), axis=1, keepdims=True) * (1.0 / tokens_all)
    aux_prob = (ALPHA * hidden * DEVS) * frac
    aux_logits = prob * (aux_prob - jnp.sum(prob * aux_prob, axis=0, keepdims=True))
    aux_part = dot(aux_logits.astype(BF16), x[...])

    wait_half(SEND_R, 0, blk, re)
    part0, loss0 = cotangents(0)
    part0 += aux_part
    loss0 += own
    send_dots(0)
    slot_grads(0, HALF)
    gxb[pl.ds(0, cap), :] = gxs[pl.ds(0, cap), :]

    wait_half(SEND_R, 1, blk, re)
    part1, loss1 = cotangents(1)
    reduced = jnp.concatenate([part0 + part1, jnp.broadcast_to(loss0 + loss1, (DEVS, LANES))], axis=1)
    for e in range(DEVS):
        red_s[e] = reduced[e:e + 1]
    red_r[0] = red_s[me]
    for p in orders[1] + orders[0]:
        remote(SEND_RS, p, red_s.at[pl.ds(peer(p), 1)], row(red_r, p)).start()
    send_dots(1)
    send_back((1, 2, 3, 5, 6, 7, 4))
    slot_grads(8, 4)
    send_back((11, 8, 9, 10))
    slot_grads(12, 4)

    for c in range(2):
        wait_half(SEND_RS, c, row, red_r)
    total = tree_sum([red_r[p] for p in range(DEVS)])
    row_s[0] = total[:, :hidden]
    row_r[0] = total[:, :hidden]
    for p in orders[1] + orders[0]:
        remote(SEND_AG, p, row(row_s, 0), row(row_r, p)).start()
    send_back((15, 12, 13, 14))
    aux = DEVS * jnp.sum(frac * mean_prob, axis=0, keepdims=True)
    loss = total[:, hidden:hidden + 1] * (1.0 / numel) + ALPHA * aux
    loss_ref[...] = jnp.broadcast_to(loss, loss_ref.shape)

    @pl.loop(0, tiles, unroll=2)
    def _(n):
        cols = pl.ds(pl.multiple_of(n * wide, wide), wide)
        dw2_ref[cols, :] = dot(actt[cols, :], gy[...]).astype(BF16)

    @pl.loop(0, dw1_ref.shape[0])
    def _(n):
        dw1_ref[n] = dot(xet[...], dpre[:, pl.ds(pl.multiple_of(n * wide, wide), wide)]).astype(BF16)

    for c in range(2):
        wait_half(SEND_DOT, c, row, dot_r)
    dots = rows_of(dot_r, range(DEVS), LANES).astype(BF16)
    at = lambda pos, keep: (place == jnp.where(keep, pos, -1)).astype(F32).astype(BF16)
    grad1 = jnp.sum(where(block1 == expert, dot(dots, at(pos1, keep1))), axis=0, keepdims=True)
    grad2 = jnp.sum(where(block2 == expert, dot(dots, at(pos2, keep2))), axis=0, keepdims=True)
    dlogits = aux_logits + gamma * (grad1 - grad2) * (hot1 - hot2)
    dlog_pad = jnp.concatenate([dlogits, jnp.zeros((LANES - DEVS, seq), F32)], axis=0)
    gate_pad = jnp.concatenate([wg[...], jnp.zeros((LANES - DEVS, hidden), BF16)], axis=0)
    base[...] = r[...].astype(F32) + dot(jnp.transpose(dlog_pad).astype(BF16), gate_pad)
    for c in range(2):
        wait_half(SEND_GX, c, blk, gxb)
    for c in range(2):
        wait_half(SEND_AG, c, row, row_r)
    gw_ref[...] = rows_of(row_r, [peer(p) for p in range(DEVS)], hidden)

    for kind, view in ((SEND_X, blk(xs, 1, 15)), (SEND_R, blk(rs, 1, 15)), (SEND_GX, blk(gxs, 1, 15)),
                       (SEND_MSG, row(msg_s, 1, 15)), (SEND_DOT, row(dot_s, 1, 15)),
                       (SEND_RS, row(red_s, 1, 15)), (SEND_AG, row(row_r, 1, 15))):
        remote(kind, 1, view, view).wait_send()


def store_kernel(loss, gw, dw2, dw1, xet, dpre, dispt, gxb, base,
                 loss_out, gx_out, dw1_out, dw2_out, gw_out, gx, tiles, loss_buf, sem):
    done, _, wide = dw1.shape
    more = tiles.shape[0]
    tile = lambda n: pl.ds(n * wide, wide)
    pairs = [(dw2, dw2_out), (gw, gw_out)] + [(dw1.at[n], dw1_out.at[:, tile(n)]) for n in range(done)]
    pairs += [(tiles.at[n], dw1_out.at[:, tile(done + n)]) for n in range(more)] + [(gx, gx_out), (loss_buf, loss_out)]
    copies = [pltpu.make_async_copy(src, dst, sem.at[i]) for i, (src, dst) in enumerate(pairs)]
    for copy in copies[:2 + done]:
        copy.start()
    loss_buf[0, 0] = jnp.max(loss[...])
    copies[-1].start()
    for n in range(more):
        tiles[n] = dot(xet[...], dpre[:, tile(done + n)]).astype(BF16)
        copies[2 + done + n].start()
    gx[...] = (base[...] + dot(dispt[...], gxb[...])).astype(BF16)
    copies[-2].start()
    for copy in copies:
        copy.wait()


def solution(mesh):
    def layer_body(x_loc, r_loc, w_gate, w_in_loc, w_out_loc, first_ids, second_ids, keep_ids):
        _, seq, hidden = x_loc.shape
        ff = w_in_loc.shape[2]
        cap = 2 * seq // DEVS
        slots = DEVS * cap
        anyspace = pl.BlockSpec(memory_space=pl.ANY)
        vmem = pl.BlockSpec(memory_space=pltpu.VMEM)
        wide, early = 512, 4
        late = ff // wide - early
        results = pl.pallas_call(
            functools.partial(layer_kernel, cap),
            out_shape=(
                pltpu.VMEM((8, LANES), F32),
                pltpu.VMEM((DEVS, hidden), F32),
                pltpu.VMEM((ff, hidden), BF16),
                pltpu.VMEM((early, hidden, wide), BF16),
                pltpu.VMEM((hidden, slots), BF16),
                pltpu.VMEM((slots, ff), BF16),
                pltpu.VMEM((seq, slots), BF16),
                pltpu.VMEM((slots, hidden), BF16),
                pltpu.VMEM((seq, hidden), F32),
            ),
            in_specs=[anyspace] * 8,
            out_specs=(vmem,) * 9,
            scratch_shapes=[
                pltpu.VMEM((seq, hidden), BF16),
                pltpu.VMEM((seq, hidden), BF16),
                pltpu.VMEM((DEVS, hidden), BF16),
                pltpu.VMEM((hidden, ff), BF16),
                pltpu.VMEM((ff, hidden), BF16),
                pltpu.VMEM((ff, hidden), BF16),
                pltpu.VMEM((hidden, ff), BF16),
                pltpu.VMEM((3 + PAD, 1, seq), jnp.int32),
                pltpu.VMEM((slots, seq), BF16),
                pltpu.VMEM((slots, hidden), BF16),
                pltpu.VMEM((slots, hidden), BF16),
                pltpu.VMEM((slots, hidden), BF16),
                pltpu.VMEM((slots, hidden), BF16),
                pltpu.VMEM((slots, hidden), BF16),
                pltpu.VMEM((2, HALF * cap, 512), F32),
                pltpu.VMEM((slots, ff), BF16),
                pltpu.VMEM((ff, slots), BF16),
                pltpu.VMEM((HALF * cap, hidden), F32),
                pltpu.VMEM((slots, ff), F32),
                pltpu.VMEM((slots, hidden), BF16),
                pltpu.VMEM((slots, hidden), BF16),
                pltpu.VMEM((DEVS + PAD, 1, LANES), F32),
                pltpu.VMEM((DEVS + PAD, 1, LANES), F32),
                pltpu.VMEM((DEVS + PAD, 1, LANES), F32),
                pltpu.VMEM((DEVS + PAD, 1, LANES), F32),
                pltpu.VMEM((DEVS + PAD, 1, hidden + LANES), F32),
                pltpu.VMEM((DEVS + PAD, 1, hidden + LANES), F32),
                pltpu.VMEM((1 + PAD, 1, hidden), F32),
                pltpu.VMEM((DEVS + PAD, 1, hidden), F32),
                pltpu.SemaphoreType.DMA((6,)),
                pltpu.SemaphoreType.DMA((7,)),
                pltpu.SemaphoreType.DMA((7, 2)),
            ],
            compiler_params=pltpu.CompilerParams(
                collective_id=0, has_side_effects=True, vmem_limit_bytes=48 * 1024 * 1024),
            name="moe_layer",
        )(x_loc[0], r_loc[0], w_gate.T, w_in_loc[0], w_out_loc[0], first_ids, second_ids, keep_ids)
        loss, gx, dw1, dw2, gw = pl.pallas_call(
            store_kernel,
            out_shape=(
                jax.ShapeDtypeStruct((1, 1), F32),
                jax.ShapeDtypeStruct((seq, hidden), BF16),
                jax.ShapeDtypeStruct((hidden, ff), BF16),
                jax.ShapeDtypeStruct((ff, hidden), BF16),
                jax.ShapeDtypeStruct((DEVS, hidden), F32),
            ),
            in_specs=[vmem] * 9,
            out_specs=(anyspace,) * 5,
            scratch_shapes=[
                pltpu.VMEM((seq, hidden), BF16),
                pltpu.VMEM((late, hidden, wide), BF16),
                pltpu.SMEM((1, 1), F32),
                pltpu.SemaphoreType.DMA((4 + ff // wide,)),
            ],
            compiler_params=pltpu.CompilerParams(vmem_limit_bytes=12 * 1024 * 1024),
            name="store_results",
        )(*results)
        return loss.reshape(()), gx[None], dw1[None], dw2[None], gw.T

    row_spec = P('ep', None, None)
    id_spec = P('ep', None)
    return jax.shard_map(layer_body, mesh=mesh, in_specs=(row_spec, row_spec, P(None, None), row_spec, row_spec, id_spec, id_spec, id_spec), out_specs=(P(), row_spec, row_spec, row_spec, P(None, None)), check_vma=False)
```

```python
import functools

import jax
import jax.numpy as jnp
from jax import lax
from jax.experimental import pallas as pl
from jax.experimental.pallas import tpu as pltpu
from jax.sharding import PartitionSpec as P

ALPHA = 0.01
MESH = pl.DeviceIdType.MESH
F32 = jnp.float32
BF16 = jnp.bfloat16

DEVS = 16
LANES = 128
PAD = 8
PART = 4

SEND_X, SEND_R, SEND_MSG, SEND_DOT, SEND_GX, SEND_RS, SEND_AG = range(7)


def offset_of(p):
    x, y, core = p & 1, (p >> 1) & 1, (p >> 2) & 1
    z = x ^ y ^ (p >> 3)
    return core | (x << 1) | (y << 2) | (z << 3)


def block_of(ids, me):
    k = jnp.bitwise_xor(ids, me)
    core, x, y, z = [(k >> i) & 1 for i in range(4)]
    return x + 2 * y + 4 * core + 8 * (x ^ y ^ z)


def dot(a, b, ca=1, cb=0):
    return lax.dot_general(a, b, (((ca,), (cb,)), ((), ())), preferred_element_type=F32)


def iota(shape, axis):
    return lax.broadcasted_iota(jnp.int32, shape, axis)


def where(mask, value):
    return jnp.where(mask, value, jnp.zeros_like(value))


def tree_sum(rows):
    rows = list(rows)
    while len(rows) > 1:
        rows = [rows[i] + rows[i + 1] for i in range(0, len(rows), 2)]
    return rows[0]


def rows_of(ref, places, width):
    n = len(places)
    out = jnp.zeros((n, width), F32)
    sub = iota((n, width), 0)
    for i, place in enumerate(places):
        out = jnp.where(sub == place, jnp.broadcast_to(ref[i], (n, width)), out)
    return out


def split3(values):
    high = values.astype(BF16)
    rest = values - high.astype(F32)
    mid = rest.astype(BF16)
    return high, mid, (rest - mid.astype(F32)).astype(BF16)


def layer_kernel(cap, x_hbm, r_hbm, wg_hbm, w1_hbm, w2_hbm, e1_hbm, e2_hbm, k2_hbm,
                 loss_ref, gw_ref, dw2_ref, dw1_ref, xet, dpre, dispt, gxb, base,
                 x, r, wg, w1, w2, w1t, w2t, ids, disp, xs, rs, xe, re, gy, pre, act, actt, acc, slope, ybuf, gxs,
                 msg_s, msg_r, dot_s, dot_r, red_s, red_r, row_s, row_r,
                 local_sem, send_sem, recv_sem):
    seq, hidden = x.shape
    ff = w1.shape[1]
    part_rows = PART * cap
    parts = range(DEVS // PART)
    tokens_all = DEVS * seq
    numel = tokens_all * hidden

    me = lax.axis_index("ep")
    bits = [lax.rem(me // (1 << i), 2) for i in range(4)]

    def peer(p):
        k = offset_of(p)
        return sum(((1 - bits[i]) if (k >> i) & 1 else bits[i]) * (1 << i) for i in range(4))

    def remote(kind, p, src, dst):
        return pltpu.make_async_remote_copy(
            src_ref=src, dst_ref=dst, send_sem=send_sem.at[kind], recv_sem=recv_sem.at[kind, p // PART],
            device_id=(peer(p),), device_id_type=MESH)

    others = range(1, DEVS)
    orders = ((1, 2, 3), (5, 6, 7, 4), (11, 8, 9, 10), (15, 12, 13, 14))
    far_first = orders[3] + orders[2] + orders[1] + orders[0]
    blk = lambda ref, p, n=1: ref.at[pl.ds(p * cap, n * cap), :]
    row = lambda ref, p, n=1: ref.at[pl.ds(p, n)]

    def wait_part(kind, c, part, ref):
        view = part(ref, min(orders[c]), len(orders[c]))
        remote(kind, orders[c][0], view, view).wait_recv()

    def wait_all(kind, part, ref):
        for c in parts:
            wait_part(kind, c, part, ref)

    id_copies = [pltpu.make_async_copy(src, ids.at[i], local_sem.at[0]) for i, src in enumerate((e1_hbm, e2_hbm, k2_hbm))]
    id_wait = pltpu.make_async_copy(row(ids, 0, 3), row(ids, 0, 3), local_sem.at[0])
    x_copy, r_copy, wg_copy, w1_copy, w2_copy = [
        pltpu.make_async_copy(src, dst, local_sem.at[1 + i]) for i, (src, dst) in enumerate((
            (x_hbm, x), (r_hbm, r), (wg_hbm, wg), (w1_hbm, w1), (w2_hbm, w2)))]
    barrier = pltpu.get_barrier_semaphore()
    for p in others:
        pl.semaphore_signal(barrier, inc=1, device_id=(peer(p),), device_id_type=MESH)
    for copy in id_copies + [x_copy, r_copy, wg_copy, w1_copy, w2_copy]:
        copy.start()

    expert = iota((DEVS, seq), 0)
    earlier = (iota((seq, seq), 0) < iota((seq, seq), 1)).astype(F32).astype(BF16)
    id_wait.wait()
    e1, e2, k2 = ids[0], ids[1], ids[2]
    hot1 = (e1 == expert).astype(F32)
    hot2 = (e2 == expert).astype(F32)
    kept2 = hot2 * k2.astype(F32)
    before = dot(jnp.concatenate([hot1, kept2], axis=0).astype(BF16), earlier)
    count1 = jnp.sum(hot1, axis=1, keepdims=True)
    pos1 = jnp.sum(before[:DEVS] * hot1, axis=0, keepdims=True).astype(jnp.int32)
    pos2 = jnp.sum((before[DEVS:] + count1) * hot2, axis=0, keepdims=True).astype(jnp.int32)
    keep1 = pos1 < cap
    keep2 = (pos2 < cap) & (k2 > 0)
    block1, block2 = block_of(e1, me), block_of(e2, me)
    slot1 = jnp.where(keep1, block1 * cap + pos1, -1)
    slot2 = jnp.where(keep2, block2 * cap + pos2, -1)

    rows_in = [pl.ds(c * part_rows, part_rows) for c in parts]

    def dispatch_x(c):
        slot = iota((part_rows, seq), 0) + c * part_rows
        table = ((slot == slot1) | (slot == slot2)).astype(F32).astype(BF16)
        disp[rows_in[c], :] = table
        xs[rows_in[c], :] = dot(table, x[...]).astype(BF16)

    def dispatch_r(c):
        rs[rows_in[c], :] = dot(disp[rows_in[c], :], r[...]).astype(BF16)

    def send_blocks(kind, c, src, dst):
        for p in orders[c]:
            remote(kind, p, blk(src, p), blk(dst, p)).start()

    x_copy.wait()
    dispatch_x(0)
    pl.semaphore_wait(barrier, DEVS - 1)
    send_blocks(SEND_X, 0, xs, xe)
    xe[pl.ds(0, cap), :] = xs[pl.ds(0, cap), :]
    dispatch_x(1)
    send_blocks(SEND_X, 1, xs, xe)
    r_copy.wait()
    dispatch_r(0)
    wg_copy.wait()
    logits = dot(wg[...], x[...], 1, 1)
    shifted = jnp.exp(logits - jnp.max(logits, axis=0, keepdims=True))
    prob = shifted / jnp.sum(shifted, axis=0, keepdims=True)
    gate1 = jnp.sum(prob * hot1, axis=0, keepdims=True)
    gate2 = jnp.sum(prob * hot2, axis=0, keepdims=True)
    gate_sum = gate1 + gate2
    norm1, norm2 = gate1 / gate_sum, gate2 / gate_sum
    gamma = norm1 * norm2
    place = iota((LANES, seq), 0)

    def by_slot(first, second, shift):
        n = len(first)
        total = 0.0
        for hot, values, pos, keep in ((hot1, first, pos1, keep1), (hot2, second, pos2, keep2)):
            table = (place == jnp.where(keep, pos + shift, -1)).astype(F32).astype(BF16)
            stack = jnp.concatenate([hot * v.astype(F32) for v in values], axis=0).astype(BF16)
            total += dot(stack, table, 1, 1)
        return sum(total[i * DEVS:(i + 1) * DEVS] for i in range(n))

    gamma_parts = split3(gamma)
    message = by_slot([norm1.astype(BF16)], [norm2.astype(BF16)], 0)
    message += by_slot(gamma_parts, gamma_parts, cap) + by_slot([e2], [e1], 2 * cap)
    prob_sum = jnp.sum(prob, axis=1, keepdims=True)
    sub, lane = iota((DEVS, LANES), 0), iota((DEVS, LANES), 1)
    count_lane, prob_lane = lane == sub + 3 * cap, lane == sub + 3 * cap + DEVS
    stats = where(count_lane, jnp.broadcast_to(count1, (DEVS, LANES)))
    stats += where(prob_lane, jnp.broadcast_to(prob_sum, (DEVS, LANES)))
    message += jnp.sum(stats, axis=0, keepdims=True)
    for e in range(DEVS):
        msg_s[e] = message[e:e + 1]
    msg_r[0] = msg_s[me]
    for p in far_first:
        remote(SEND_MSG, p, msg_s.at[pl.ds(peer(p), 1)], row(msg_r, p)).start()
    send_blocks(SEND_R, 0, rs, re)
    re[pl.ds(0, cap), :] = rs[pl.ds(0, cap), :]
    for c in (1, 2):
        dispatch_x(c + 1)
        send_blocks(SEND_X, c + 1, xs, xe)
        dispatch_r(c)
        send_blocks(SEND_R, c, rs, re)
    dispatch_r(3)
    send_blocks(SEND_R, 3, rs, re)
    dispt[...] = jnp.transpose(disp[...])
    own = jnp.sum(jnp.sum(x[...].astype(F32) * r[...].astype(F32), axis=0, keepdims=True), axis=1, keepdims=True)

    wide = 512
    tiles = ff // wide
    tile = lambda n: pl.ds(n * wide, wide)
    lane_of, slot_of = iota((part_rows, LANES), 1), lax.rem(iota((part_rows, LANES), 0), cap)

    def forward(c):
        rows = rows_in[c]
        xet[:, rows] = jnp.transpose(xe[rows, :])
        for n in range(tiles + 2):
            if n < tiles:
                pre[n % 2] = dot(xe[rows, :], w1[:, tile(n)])
                if c == 0:
                    w2t[:, tile(n)] = jnp.transpose(w2[tile(n), :])
                elif c == 1:
                    w1t[tile(n), :] = jnp.transpose(w1[:, tile(n)])
            if 1 <= n <= tiles:
                m = n - 1
                v = pre[m % 2]
                sq = v * v
                root = 0.7978845608028654
                t = jnp.tanh(v * (root + root * 0.044715 * sq))
                hx = 0.5 * v
                a = (hx + hx * t).astype(BF16)
                act[rows, tile(m)] = a
                actt[tile(m), rows] = jnp.transpose(a)
                slope[rows, tile(m)] = (0.5 + 0.5 * t) + hx * (1.0 - t * t) * (root + 3.0 * root * 0.044715 * sq)
            if n >= 2:
                m = n - 2
                y = dot(act[rows, tile(m)], w2[tile(m), :])
                if m:
                    y += acc[...]
                if m < tiles - 1:
                    acc[...] = y
                else:
                    ybuf[rows, :] = y.astype(BF16)

    def cotangents(c):
        rows = rows_in[c]
        mine = range(c * PART, (c + 1) * PART)
        spread = jnp.concatenate([jnp.broadcast_to(msg_r[p], (cap, LANES)) for p in mine], axis=0)
        column = lambda i: jnp.sum(where(lane_of == slot_of + i * cap, spread), axis=1, keepdims=True)
        weight, scale, other = column(0), column(1), column(2)
        r_rows = re[rows, :].astype(F32)
        gy[rows, :] = (r_rows * weight).astype(BF16)
        dots = jnp.sum(r_rows * ybuf[rows, :].astype(F32), axis=1, keepdims=True)
        dot_mat = where(lane_of == slot_of, jnp.broadcast_to(dots, (part_rows, LANES)))
        for p in mine:
            q = (p - c * PART) * cap
            (dot_s if p else dot_r)[p] = jnp.sum(dot_mat[q:q + cap], axis=0, keepdims=True)
        share = jnp.broadcast_to(dots.astype(BF16).astype(F32) * scale, (part_rows, LANES))
        table = where(lane_of == me, share) - where(lane_of == other.astype(jnp.int32), share)
        part = dot(jnp.transpose(table).astype(BF16), xe[rows, :])[:DEVS]
        return part, jnp.sum(weight * dots, axis=0, keepdims=True)

    def slot_grads(c):
        rows = rows_in[c]
        for n in range(tiles):
            da = dot(gy[rows, :], w2t[:, tile(n)]).astype(BF16).astype(F32)
            dpre[rows, tile(n)] = (da * slope[rows, tile(n)]).astype(BF16)
        gxs[rows, :] = dot(dpre[rows, :], w1t[...]).astype(BF16)

    def send_dots(c):
        for p in orders[c]:
            remote(SEND_DOT, p, row(dot_s, p), row(dot_r, p)).start()

    w1_copy.wait()
    w2_copy.wait()

    def forward_part(c):
        wait_part(SEND_X, c, blk, xe)
        forward(c)

    def router_aux():
        wait_all(SEND_MSG, row, msg_r)
        totals = jnp.broadcast_to(tree_sum([msg_r[p] for p in range(DEVS)]), (DEVS, LANES))
        frac = jnp.sum(where(count_lane, totals), axis=1, keepdims=True) * (1.0 / tokens_all)
        mean_prob = jnp.sum(where(prob_lane, totals), axis=1, keepdims=True) * (1.0 / tokens_all)
        aux_prob = (ALPHA * hidden * DEVS) * frac
        aux_logits = prob * (aux_prob - jnp.sum(prob * aux_prob, axis=0, keepdims=True))
        return frac, mean_prob, aux_logits

    def backward_part(c, gate_part, loss_part):
        wait_part(SEND_R, c, blk, re)
        gate_c, loss_c = cotangents(c)
        gate_part, loss_part = gate_part + gate_c, loss_part + loss_c
        if c == 3:
            reduced = jnp.concatenate([gate_part, jnp.broadcast_to(loss_part, (DEVS, LANES))], axis=1)
            for e in range(DEVS):
                red_s[e] = reduced[e:e + 1]
            red_r[0] = red_s[me]
            for p in far_first:
                remote(SEND_RS, p, red_s.at[pl.ds(peer(p), 1)], row(red_r, p)).start()
            send_dots(c)
            send_blocks(SEND_GX, 2, gxs, gxb)
        slot_grads(c)
        if c == 0:
            gxb[pl.ds(0, cap), :] = gxs[pl.ds(0, cap), :]
        if c != 2:
            send_blocks(SEND_GX, c, gxs, gxb)
        if c != 3:
            send_dots(c)
        return gate_part, loss_part

    forward_part(0)
    forward_part(1)
    frac, mean_prob, aux_logits = router_aux()
    sums = dot(aux_logits.astype(BF16), x[...]), own
    sums = backward_part(0, *sums)
    for c in (1, 2):
        forward_part(c + 1)
        sums = backward_part(c, *sums)
    backward_part(3, *sums)

    def grad_w2(n):
        cols = pl.ds(pl.multiple_of(n * wide, wide), wide)
        dw2_ref[cols, :] = dot(actt[cols, :], gy[...]).astype(BF16)

    pl.loop(0, 4, unroll=2)(grad_w2)

    wait_all(SEND_RS, row, red_r)
    total = tree_sum([red_r[p] for p in range(DEVS)])
    row_s[0] = total[:, :hidden]
    row_r[0] = total[:, :hidden]
    for p in far_first:
        remote(SEND_AG, p, row(row_s, 0), row(row_r, p)).start()
    aux = DEVS * jnp.sum(frac * mean_prob, axis=0, keepdims=True)
    loss = total[:, hidden:hidden + 1] * (1.0 / numel) + ALPHA * aux
    loss_ref[...] = jnp.broadcast_to(loss, loss_ref.shape)

    pl.loop(4, tiles, unroll=2)(grad_w2)

    @pl.loop(0, dw1_ref.shape[0])
    def _(n):
        dw1_ref[n] = dot(xet[...], dpre[:, pl.ds(pl.multiple_of(n * wide, wide), wide)]).astype(BF16)

    wait_all(SEND_DOT, row, dot_r)
    dots = rows_of(dot_r, range(DEVS), LANES).astype(BF16)
    at = lambda pos, keep: (place == jnp.where(keep, pos, -1)).astype(F32).astype(BF16)
    grad1 = jnp.sum(where(block1 == expert, dot(dots, at(pos1, keep1))), axis=0, keepdims=True)
    grad2 = jnp.sum(where(block2 == expert, dot(dots, at(pos2, keep2))), axis=0, keepdims=True)
    dlogits = aux_logits + gamma * (grad1 - grad2) * (hot1 - hot2)
    dlog_pad = jnp.concatenate([dlogits, jnp.zeros((LANES - DEVS, seq), F32)], axis=0)
    gate_pad = jnp.concatenate([wg[...], jnp.zeros((LANES - DEVS, hidden), BF16)], axis=0)
    base[...] = r[...].astype(F32) + dot(jnp.transpose(dlog_pad).astype(BF16), gate_pad)
    wait_all(SEND_GX, blk, gxb)
    wait_all(SEND_AG, row, row_r)
    gw_ref[...] = rows_of(row_r, [peer(p) for p in range(DEVS)], hidden)

    for kind, view in ((SEND_X, blk(xs, 1, 15)), (SEND_R, blk(rs, 1, 15)), (SEND_GX, blk(gxs, 1, 15)),
                       (SEND_MSG, row(msg_s, 1, 15)), (SEND_DOT, row(dot_s, 1, 15)),
                       (SEND_RS, row(red_s, 1, 15)), (SEND_AG, row(row_r, 1, 15))):
        remote(kind, 1, view, view).wait_send()


def store_kernel(loss, gw, dw2, dw1, xet, dpre, dispt, gxb, base,
                 loss_out, gx_out, dw1_out, dw2_out, gw_out, gx, tiles, loss_buf, sem):
    done, _, wide = dw1.shape
    more = tiles.shape[0]
    tile = lambda n: pl.ds(n * wide, wide)
    pairs = [(dw2, dw2_out), (gw, gw_out)] + [(dw1.at[n], dw1_out.at[:, tile(n)]) for n in range(done)]
    pairs += [(tiles.at[n], dw1_out.at[:, tile(done + n)]) for n in range(more)] + [(gx, gx_out), (loss_buf, loss_out)]
    copies = [pltpu.make_async_copy(src, dst, sem.at[i]) for i, (src, dst) in enumerate(pairs)]
    for copy in copies[:2 + done]:
        copy.start()
    loss_buf[0, 0] = jnp.max(loss[...])
    copies[-1].start()
    for n in range(more):
        tiles[n] = dot(xet[...], dpre[:, tile(done + n)]).astype(BF16)
        copies[2 + done + n].start()
    gx[...] = (base[...] + dot(dispt[...], gxb[...])).astype(BF16)
    copies[-2].start()
    for copy in copies:
        copy.wait()


def solution(mesh):
    def layer_body(x_loc, r_loc, w_gate, w_in_loc, w_out_loc, first_ids, second_ids, keep_ids):
        _, seq, hidden = x_loc.shape
        ff = w_in_loc.shape[2]
        cap = 2 * seq // DEVS
        slots = DEVS * cap
        anyspace = pl.BlockSpec(memory_space=pl.ANY)
        vmem = pl.BlockSpec(memory_space=pltpu.VMEM)
        wide, early = 512, 2
        late = ff // wide - early
        results = pl.pallas_call(
            functools.partial(layer_kernel, cap),
            out_shape=(
                pltpu.VMEM((8, LANES), F32),
                pltpu.VMEM((DEVS, hidden), F32),
                pltpu.VMEM((ff, hidden), BF16),
                pltpu.VMEM((early, hidden, wide), BF16),
                pltpu.VMEM((hidden, slots), BF16),
                pltpu.VMEM((slots, ff), BF16),
                pltpu.VMEM((seq, slots), BF16),
                pltpu.VMEM((slots, hidden), BF16),
                pltpu.VMEM((seq, hidden), F32),
            ),
            in_specs=[anyspace] * 8,
            out_specs=(vmem,) * 9,
            scratch_shapes=[
                pltpu.VMEM((seq, hidden), BF16),
                pltpu.VMEM((seq, hidden), BF16),
                pltpu.VMEM((DEVS, hidden), BF16),
                pltpu.VMEM((hidden, ff), BF16),
                pltpu.VMEM((ff, hidden), BF16),
                pltpu.VMEM((ff, hidden), BF16),
                pltpu.VMEM((hidden, ff), BF16),
                pltpu.VMEM((3 + PAD, 1, seq), jnp.int32),
                pltpu.VMEM((slots, seq), BF16),
                pltpu.VMEM((slots, hidden), BF16),
                pltpu.VMEM((slots, hidden), BF16),
                pltpu.VMEM((slots, hidden), BF16),
                pltpu.VMEM((slots, hidden), BF16),
                pltpu.VMEM((slots, hidden), BF16),
                pltpu.VMEM((2, PART * cap, 512), F32),
                pltpu.VMEM((slots, ff), BF16),
                pltpu.VMEM((ff, slots), BF16),
                pltpu.VMEM((PART * cap, hidden), F32),
                pltpu.VMEM((slots, ff), F32),
                pltpu.VMEM((slots, hidden), BF16),
                pltpu.VMEM((slots, hidden), BF16),
                pltpu.VMEM((DEVS + PAD, 1, LANES), F32),
                pltpu.VMEM((DEVS + PAD, 1, LANES), F32),
                pltpu.VMEM((DEVS + PAD, 1, LANES), F32),
                pltpu.VMEM((DEVS + PAD, 1, LANES), F32),
                pltpu.VMEM((DEVS + PAD, 1, hidden + LANES), F32),
                pltpu.VMEM((DEVS + PAD, 1, hidden + LANES), F32),
                pltpu.VMEM((1 + PAD, 1, hidden), F32),
                pltpu.VMEM((DEVS + PAD, 1, hidden), F32),
                pltpu.SemaphoreType.DMA((6,)),
                pltpu.SemaphoreType.DMA((7,)),
                pltpu.SemaphoreType.DMA((7, DEVS // PART)),
            ],
            compiler_params=pltpu.CompilerParams(
                collective_id=0, has_side_effects=True, vmem_limit_bytes=48 * 1024 * 1024),
            name="moe_layer",
        )(x_loc[0], r_loc[0], w_gate.T, w_in_loc[0], w_out_loc[0], first_ids, second_ids, keep_ids)
        loss, gx, dw1, dw2, gw = pl.pallas_call(
            store_kernel,
            out_shape=(
                jax.ShapeDtypeStruct((1, 1), F32),
                jax.ShapeDtypeStruct((seq, hidden), BF16),
                jax.ShapeDtypeStruct((hidden, ff), BF16),
                jax.ShapeDtypeStruct((ff, hidden), BF16),
                jax.ShapeDtypeStruct((DEVS, hidden), F32),
            ),
            in_specs=[vmem] * 9,
            out_specs=(anyspace,) * 5,
            scratch_shapes=[
                pltpu.VMEM((seq, hidden), BF16),
                pltpu.VMEM((late, hidden, wide), BF16),
                pltpu.SMEM((1, 1), F32),
                pltpu.SemaphoreType.DMA((4 + ff // wide,)),
            ],
            compiler_params=pltpu.CompilerParams(vmem_limit_bytes=12 * 1024 * 1024),
            name="store_results",
        )(*results)
        return loss.reshape(()), gx[None], dw1[None], dw2[None], gw.T

    row_spec = P('ep', None, None)
    id_spec = P('ep', None)
    return jax.shard_map(layer_body, mesh=mesh, in_specs=(row_spec, row_spec, P(None, None), row_spec, row_spec, id_spec, id_spec, id_spec), out_specs=(P(), row_spec, row_spec, row_spec, P(None, None)), check_vma=False)
```

```python
import functools

import jax
import jax.numpy as jnp
from jax import lax
from jax.experimental import pallas as pl
from jax.experimental.pallas import tpu as pltpu
from jax.sharding import PartitionSpec as P

ALPHA = 0.01
MESH = pl.DeviceIdType.MESH
F32 = jnp.float32
BF16 = jnp.bfloat16

DEVS = 16
LANES = 128
PAD = 8
PART = 4

SEND_X, SEND_R, SEND_MSG, SEND_DOT, SEND_GX, SEND_RS, SEND_AG = range(7)


def offset_of(p):
    x, y, core = p & 1, (p >> 1) & 1, (p >> 2) & 1
    z = x ^ y ^ (p >> 3)
    return core | (x << 1) | (y << 2) | (z << 3)


def block_of(ids, me):
    k = jnp.bitwise_xor(ids, me)
    core, x, y, z = [(k >> i) & 1 for i in range(4)]
    return x + 2 * y + 4 * core + 8 * (x ^ y ^ z)


def dot(a, b, ca=1, cb=0):
    return lax.dot_general(a, b, (((ca,), (cb,)), ((), ())), preferred_element_type=F32)


def iota(shape, axis):
    return lax.broadcasted_iota(jnp.int32, shape, axis)


def where(mask, value):
    return jnp.where(mask, value, jnp.zeros_like(value))


def tree_sum(rows):
    rows = list(rows)
    while len(rows) > 1:
        rows = [rows[i] + rows[i + 1] for i in range(0, len(rows), 2)]
    return rows[0]


def rows_of(ref, places, width):
    n = len(places)
    out = jnp.zeros((n, width), F32)
    sub = iota((n, width), 0)
    for i, place in enumerate(places):
        out = jnp.where(sub == place, jnp.broadcast_to(ref[i], (n, width)), out)
    return out


def split3(values):
    high = values.astype(BF16)
    rest = values - high.astype(F32)
    mid = rest.astype(BF16)
    return high, mid, (rest - mid.astype(F32)).astype(BF16)


def layer_kernel(cap, x_hbm, r_hbm, wg_hbm, w1_hbm, w2_hbm, e1_hbm, e2_hbm, k2_hbm,
                 loss_ref, gw_ref, dw2_ref, dw1_ref, xet, dpre, dispt, gxb, base,
                 x, r, wg, w1, w2, w1t, w2t, ids, disp, xs, rs, xe, re, gy, pre, act, actt, acc, slope, ybuf, gxs,
                 msg_s, msg_r, dot_s, dot_r, red_s, red_r, row_s, row_r, held, at, ahead, gate_sums, sum_ref,
                 local_sem, send_sem, recv_sem):
    seq, hidden = x.shape
    ff = w1.shape[1]
    part_rows = PART * cap
    parts = range(DEVS // PART)
    tokens_all = DEVS * seq
    numel = tokens_all * hidden

    me = lax.axis_index("ep")
    bits = [lax.rem(me // (1 << i), 2) for i in range(4)]

    def peer(p):
        k = offset_of(p)
        return sum(((1 - bits[i]) if (k >> i) & 1 else bits[i]) * (1 << i) for i in range(4))

    def remote(kind, p, src, dst):
        return pltpu.make_async_remote_copy(
            src_ref=src, dst_ref=dst, send_sem=send_sem.at[kind], recv_sem=recv_sem.at[kind, p // PART],
            device_id=(peer(p),), device_id_type=MESH)

    others = range(1, DEVS)
    orders = ((1, 2, 3), (5, 6, 7, 4), (11, 8, 9, 10), (15, 12, 13, 14))
    far_first = orders[3] + orders[2] + orders[1] + orders[0]
    blk = lambda ref, p, n=1: ref.at[pl.ds(p * cap, n * cap), :]
    row = lambda ref, p, n=1: ref.at[pl.ds(p, n)]

    def wait_part(kind, c, part, ref):
        view = part(ref, min(orders[c]), len(orders[c]))
        remote(kind, orders[c][0], view, view).wait_recv()

    def wait_all(kind, part, ref):
        for c in parts:
            wait_part(kind, c, part, ref)

    id_copies = [pltpu.make_async_copy(src, ids.at[i], local_sem.at[0]) for i, src in enumerate((e1_hbm, e2_hbm, k2_hbm))]
    id_wait = pltpu.make_async_copy(row(ids, 0, 3), row(ids, 0, 3), local_sem.at[0])
    x_copy, r_copy, wg_copy, w1_copy, w2_copy = [
        pltpu.make_async_copy(src, dst, local_sem.at[1 + i]) for i, (src, dst) in enumerate((
            (x_hbm, x), (r_hbm, r), (wg_hbm, wg), (w1_hbm, w1), (w2_hbm, w2)))]
    barrier = pltpu.get_barrier_semaphore()
    for p in others:
        pl.semaphore_signal(barrier, inc=1, device_id=(peer(p),), device_id_type=MESH)
    for copy in id_copies + [x_copy, r_copy, wg_copy, w1_copy, w2_copy]:
        copy.start()

    expert = iota((DEVS, seq), 0)
    earlier = (iota((seq, seq), 0) < iota((seq, seq), 1)).astype(F32).astype(BF16)
    id_wait.wait()
    e1, e2, k2 = ids[0], ids[1], ids[2]
    hot1 = (e1 == expert).astype(F32)
    hot2 = (e2 == expert).astype(F32)
    kept2 = hot2 * k2.astype(F32)
    before = dot(jnp.concatenate([hot1, kept2], axis=0).astype(BF16), earlier)
    count1 = jnp.sum(hot1, axis=1, keepdims=True)
    pos1 = jnp.sum(before[:DEVS] * hot1, axis=0, keepdims=True).astype(jnp.int32)
    pos2 = jnp.sum((before[DEVS:] + count1) * hot2, axis=0, keepdims=True).astype(jnp.int32)
    keep1 = pos1 < cap
    keep2 = (pos2 < cap) & (k2 > 0)
    block1, block2 = block_of(e1, me), block_of(e2, me)
    slot1 = jnp.where(keep1, block1 * cap + pos1, -1)
    slot2 = jnp.where(keep2, block2 * cap + pos2, -1)

    rows_in = [pl.ds(c * part_rows, part_rows) for c in parts]

    def dispatch_x(c):
        slot = iota((part_rows, seq), 0) + c * part_rows
        table = ((slot == slot1) | (slot == slot2)).astype(F32).astype(BF16)
        disp[rows_in[c], :] = table
        xs[rows_in[c], :] = dot(table, x[...]).astype(BF16)

    def dispatch_r(c):
        rs[rows_in[c], :] = dot(disp[rows_in[c], :], r[...]).astype(BF16)

    def send_blocks(kind, c, src, dst):
        for p in orders[c]:
            remote(kind, p, blk(src, p), blk(dst, p)).start()

    x_copy.wait()
    dispatch_x(0)
    pl.semaphore_wait(barrier, DEVS - 1)
    send_blocks(SEND_X, 0, xs, xe)
    xe[pl.ds(0, cap), :] = xs[pl.ds(0, cap), :]
    dispatch_x(1)
    send_blocks(SEND_X, 1, xs, xe)
    r_copy.wait()
    dispatch_r(0)
    wg_copy.wait()
    logits = dot(wg[...], x[...], 1, 1)
    shifted = jnp.exp(logits - jnp.max(logits, axis=0, keepdims=True))
    prob = shifted / jnp.sum(shifted, axis=0, keepdims=True)
    gate1 = jnp.sum(prob * hot1, axis=0, keepdims=True)
    gate2 = jnp.sum(prob * hot2, axis=0, keepdims=True)
    gate_sum = gate1 + gate2
    norm1, norm2 = gate1 / gate_sum, gate2 / gate_sum
    gamma = norm1 * norm2
    place = iota((LANES, seq), 0)

    def by_slot(first, second, shift):
        n = len(first)
        total = 0.0
        for hot, values, pos, keep in ((hot1, first, pos1, keep1), (hot2, second, pos2, keep2)):
            table = (place == jnp.where(keep, pos + shift, -1)).astype(F32).astype(BF16)
            stack = jnp.concatenate([hot * v.astype(F32) for v in values], axis=0).astype(BF16)
            total += dot(stack, table, 1, 1)
        return sum(total[i * DEVS:(i + 1) * DEVS] for i in range(n))

    gamma_parts = split3(gamma)
    message = by_slot([norm1.astype(BF16)], [norm2.astype(BF16)], 0)
    message += by_slot(gamma_parts, gamma_parts, cap) + by_slot([e2], [e1], 2 * cap)
    held[0] = prob
    held[1] = gamma * (hot1 - hot2)
    held[2] = (block1 == expert).astype(F32)
    held[3] = (block2 == expert).astype(F32)
    at[0] = (place == jnp.where(keep1, pos1, -1)).astype(F32).astype(BF16)
    at[1] = (place == jnp.where(keep2, pos2, -1)).astype(F32).astype(BF16)
    prob_sum = jnp.sum(prob, axis=1, keepdims=True)
    sub, lane = iota((DEVS, LANES), 0), iota((DEVS, LANES), 1)
    count_lane, prob_lane = lane == sub + 3 * cap, lane == sub + 3 * cap + DEVS
    stats = where(count_lane, jnp.broadcast_to(count1, (DEVS, LANES)))
    stats += where(prob_lane, jnp.broadcast_to(prob_sum, (DEVS, LANES)))
    message += jnp.sum(stats, axis=0, keepdims=True)
    for e in range(DEVS):
        msg_s[e] = message[e:e + 1]
    msg_r[0] = msg_s[me]
    for p in far_first:
        remote(SEND_MSG, p, msg_s.at[pl.ds(peer(p), 1)], row(msg_r, p)).start()
    send_blocks(SEND_R, 0, rs, re)
    re[pl.ds(0, cap), :] = rs[pl.ds(0, cap), :]
    for c in (1, 2):
        dispatch_x(c + 1)
        send_blocks(SEND_X, c + 1, xs, xe)
        dispatch_r(c)
        send_blocks(SEND_R, c, rs, re)
    dispatch_r(3)
    send_blocks(SEND_R, 3, rs, re)
    dispt[...] = jnp.transpose(disp[...])
    own = jnp.sum(jnp.sum(x[...].astype(F32) * r[...].astype(F32), axis=0, keepdims=True), axis=1, keepdims=True)
    sum_ref[...] = jnp.broadcast_to(own, sum_ref.shape)

    wide = 512
    tiles = ff // wide
    tile = lambda n: pl.ds(n * wide, wide)
    ahead[...] = iota((part_rows, LANES), 1) - lax.rem(iota((part_rows, LANES), 0), cap)

    def forward(c):
        rows = rows_in[c]
        xet[:, rows] = jnp.transpose(xe[rows, :])
        for n in range(tiles + 2):
            if n < tiles:
                pre[n % 2] = dot(xe[rows, :], w1[:, tile(n)])
                if c == 0:
                    w2t[:, tile(n)] = jnp.transpose(w2[tile(n), :])
                elif c == 1:
                    w1t[tile(n), :] = jnp.transpose(w1[:, tile(n)])
            if 1 <= n <= tiles:
                m = n - 1
                v = pre[m % 2]
                sq = v * v
                root = 0.7978845608028654
                t = jnp.tanh(v * (root + root * 0.044715 * sq))
                hx = 0.5 * v
                a = (hx + hx * t).astype(BF16)
                act[rows, tile(m)] = a
                actt[tile(m), rows] = jnp.transpose(a)
                slope[rows, tile(m)] = (0.5 + 0.5 * t) + hx * (1.0 - t * t) * (root + 3.0 * root * 0.044715 * sq)
            if n >= 2:
                m = n - 2
                y = dot(act[rows, tile(m)], w2[tile(m), :])
                if m:
                    y += acc[...]
                if m < tiles - 1:
                    acc[...] = y
                else:
                    ybuf[rows, :] = y.astype(BF16)

    def cotangents(c):
        rows = rows_in[c]
        mine = range(c * PART, (c + 1) * PART)
        spread = jnp.concatenate([jnp.broadcast_to(msg_r[p], (cap, LANES)) for p in mine], axis=0)
        lane_of = iota((part_rows, LANES), 1)
        column = lambda i: jnp.sum(where(ahead[...] == i * cap, spread), axis=1, keepdims=True)
        weight, scale, other = column(0), column(1), column(2)
        r_rows = re[rows, :].astype(F32)
        gy[rows, :] = (r_rows * weight).astype(BF16)
        dots = jnp.sum(r_rows * ybuf[rows, :].astype(F32), axis=1, keepdims=True)
        dot_mat = where(ahead[...] == 0, jnp.broadcast_to(dots, (part_rows, LANES)))
        for p in mine:
            q = (p - c * PART) * cap
            (dot_s if p else dot_r)[p] = jnp.sum(dot_mat[q:q + cap], axis=0, keepdims=True)
        share = jnp.broadcast_to(dots.astype(BF16).astype(F32) * scale, (part_rows, LANES))
        table = where(lane_of == me, share) - where(lane_of == other.astype(jnp.int32), share)
        gate_sums[...] += dot(jnp.transpose(table).astype(BF16), xe[rows, :])[:DEVS]
        sum_ref[...] += jnp.broadcast_to(jnp.sum(weight * dots, axis=0, keepdims=True), sum_ref.shape)

    def slot_grads(c):
        rows = rows_in[c]
        for n in range(tiles):
            da = dot(gy[rows, :], w2t[:, tile(n)]).astype(BF16).astype(F32)
            dpre[rows, tile(n)] = (da * slope[rows, tile(n)]).astype(BF16)
        gxs[rows, :] = dot(dpre[rows, :], w1t[...]).astype(BF16)

    def send_dots(c):
        for p in orders[c]:
            remote(SEND_DOT, p, row(dot_s, p), row(dot_r, p)).start()

    w1_copy.wait()
    w2_copy.wait()

    def forward_part(c):
        wait_part(SEND_X, c, blk, xe)
        forward(c)

    def router_aux():
        wait_all(SEND_MSG, row, msg_r)
        sub, lane = iota((DEVS, LANES), 0), iota((DEVS, LANES), 1)
        totals = jnp.broadcast_to(tree_sum([msg_r[p] for p in range(DEVS)]), (DEVS, LANES))
        mean = lambda i: jnp.sum(where(lane == sub + i, totals), axis=1, keepdims=True) * (1.0 / tokens_all)
        frac, mean_prob = mean(3 * cap), mean(3 * cap + DEVS)
        aux = DEVS * jnp.sum(frac * mean_prob, axis=0, keepdims=True)
        loss_ref[...] = jnp.broadcast_to(ALPHA * aux, loss_ref.shape)
        aux_prob = (ALPHA * hidden * DEVS) * frac
        prob = held[0]
        aux_logits = prob * (aux_prob - jnp.sum(prob * aux_prob, axis=0, keepdims=True))
        held[0] = aux_logits
        gate_sums[...] = dot(aux_logits.astype(BF16), x[...])

    def take_rows(c):
        wait_part(SEND_R, c, blk, re)
        cotangents(c)

    def send_sums():
        reduced = jnp.concatenate([gate_sums[...], jnp.broadcast_to(sum_ref[0:1], (DEVS, LANES))], axis=1)
        for e in range(DEVS):
            red_s[e] = reduced[e:e + 1]
        red_r[0] = red_s[me]
        for p in far_first:
            remote(SEND_RS, p, red_s.at[pl.ds(peer(p), 1)], row(red_r, p)).start()

    forward_part(0)
    forward_part(1)
    router_aux()
    take_rows(0)
    slot_grads(0)
    send_blocks(SEND_GX, 0, gxs, gxb)
    gxb[pl.ds(0, cap), :] = gxs[pl.ds(0, cap), :]
    send_dots(0)
    forward_part(2)
    take_rows(1)
    slot_grads(1)
    send_blocks(SEND_GX, 1, gxs, gxb)
    send_dots(1)
    forward_part(3)
    take_rows(2)
    take_rows(3)
    send_sums()
    send_dots(2)
    send_dots(3)
    slot_grads(2)
    send_blocks(SEND_GX, 2, gxs, gxb)
    slot_grads(3)
    send_blocks(SEND_GX, 3, gxs, gxb)

    def grad_w2(n):
        cols = pl.ds(pl.multiple_of(n * wide, wide), wide)
        dw2_ref[cols, :] = dot(actt[cols, :], gy[...]).astype(BF16)

    pl.loop(0, 4, unroll=2)(grad_w2)

    wait_all(SEND_RS, row, red_r)
    total = tree_sum([red_r[p] for p in range(DEVS)])
    row_s[0] = total[:, :hidden]
    row_r[0] = total[:, :hidden]
    for p in far_first:
        remote(SEND_AG, p, row(row_s, 0), row(row_r, p)).start()
    loss_ref[...] += jnp.broadcast_to(total[:, hidden:hidden + 1] * (1.0 / numel), loss_ref.shape)

    pl.loop(4, tiles, unroll=2)(grad_w2)

    @pl.loop(0, dw1_ref.shape[0])
    def _(n):
        dw1_ref[n] = dot(xet[...], dpre[:, pl.ds(pl.multiple_of(n * wide, wide), wide)]).astype(BF16)

    wait_all(SEND_DOT, row, dot_r)
    dots = rows_of(dot_r, range(DEVS), LANES).astype(BF16)
    grad1 = jnp.sum(held[2] * dot(dots, at[0]), axis=0, keepdims=True)
    grad2 = jnp.sum(held[3] * dot(dots, at[1]), axis=0, keepdims=True)
    dlogits = held[0] + held[1] * (grad1 - grad2)
    dlog_pad = jnp.concatenate([dlogits, jnp.zeros((LANES - DEVS, seq), F32)], axis=0)
    gate_pad = jnp.concatenate([wg[...], jnp.zeros((LANES - DEVS, hidden), BF16)], axis=0)
    base[...] = r[...].astype(F32) + dot(jnp.transpose(dlog_pad).astype(BF16), gate_pad)
    wait_all(SEND_GX, blk, gxb)
    wait_all(SEND_AG, row, row_r)
    gw_ref[...] = rows_of(row_r, [peer(p) for p in range(DEVS)], hidden)

    for kind, view in ((SEND_X, blk(xs, 1, 15)), (SEND_R, blk(rs, 1, 15)), (SEND_GX, blk(gxs, 1, 15)),
                       (SEND_MSG, row(msg_s, 1, 15)), (SEND_DOT, row(dot_s, 1, 15)),
                       (SEND_RS, row(red_s, 1, 15)), (SEND_AG, row(row_r, 1, 15))):
        remote(kind, 1, view, view).wait_send()


def store_kernel(loss, gw, dw2, dw1, xet, dpre, dispt, gxb, base,
                 loss_out, gx_out, dw1_out, dw2_out, gw_out, gx, tiles, loss_buf, sem):
    done, _, wide = dw1.shape
    more = tiles.shape[0]
    tile = lambda n: pl.ds(n * wide, wide)
    pairs = [(dw2, dw2_out), (gw, gw_out)] + [(dw1.at[n], dw1_out.at[:, tile(n)]) for n in range(done)]
    pairs += [(tiles.at[n], dw1_out.at[:, tile(done + n)]) for n in range(more)] + [(gx, gx_out), (loss_buf, loss_out)]
    copies = [pltpu.make_async_copy(src, dst, sem.at[i]) for i, (src, dst) in enumerate(pairs)]
    for copy in copies[:2 + done]:
        copy.start()
    loss_buf[0, 0] = jnp.max(loss[...])
    copies[-1].start()
    for n in range(more):
        tiles[n] = dot(xet[...], dpre[:, tile(done + n)]).astype(BF16)
        copies[2 + done + n].start()
    gx[...] = (base[...] + dot(dispt[...], gxb[...])).astype(BF16)
    copies[-2].start()
    for copy in copies:
        copy.wait()


def solution(mesh):
    def layer_body(x_loc, r_loc, w_gate, w_in_loc, w_out_loc, first_ids, second_ids, keep_ids):
        _, seq, hidden = x_loc.shape
        ff = w_in_loc.shape[2]
        cap = 2 * seq // DEVS
        slots = DEVS * cap
        anyspace = pl.BlockSpec(memory_space=pl.ANY)
        vmem = pl.BlockSpec(memory_space=pltpu.VMEM)
        wide, early = 512, 2
        late = ff // wide - early
        results = pl.pallas_call(
            functools.partial(layer_kernel, cap),
            out_shape=(
                pltpu.VMEM((8, LANES), F32),
                pltpu.VMEM((DEVS, hidden), F32),
                pltpu.VMEM((ff, hidden), BF16),
                pltpu.VMEM((early, hidden, wide), BF16),
                pltpu.VMEM((hidden, slots), BF16),
                pltpu.VMEM((slots, ff), BF16),
                pltpu.VMEM((seq, slots), BF16),
                pltpu.VMEM((slots, hidden), BF16),
                pltpu.VMEM((seq, hidden), F32),
            ),
            in_specs=[anyspace] * 8,
            out_specs=(vmem,) * 9,
            scratch_shapes=[
                pltpu.VMEM((seq, hidden), BF16),
                pltpu.VMEM((seq, hidden), BF16),
                pltpu.VMEM((DEVS, hidden), BF16),
                pltpu.VMEM((hidden, ff), BF16),
                pltpu.VMEM((ff, hidden), BF16),
                pltpu.VMEM((ff, hidden), BF16),
                pltpu.VMEM((hidden, ff), BF16),
                pltpu.VMEM((3 + PAD, 1, seq), jnp.int32),
                pltpu.VMEM((slots, seq), BF16),
                pltpu.VMEM((slots, hidden), BF16),
                pltpu.VMEM((slots, hidden), BF16),
                pltpu.VMEM((slots, hidden), BF16),
                pltpu.VMEM((slots, hidden), BF16),
                pltpu.VMEM((slots, hidden), BF16),
                pltpu.VMEM((2, PART * cap, 512), F32),
                pltpu.VMEM((slots, ff), BF16),
                pltpu.VMEM((ff, slots), BF16),
                pltpu.VMEM((PART * cap, hidden), F32),
                pltpu.VMEM((slots, ff), F32),
                pltpu.VMEM((slots, hidden), BF16),
                pltpu.VMEM((slots, hidden), BF16),
                pltpu.VMEM((DEVS + PAD, 1, LANES), F32),
                pltpu.VMEM((DEVS + PAD, 1, LANES), F32),
                pltpu.VMEM((DEVS + PAD, 1, LANES), F32),
                pltpu.VMEM((DEVS + PAD, 1, LANES), F32),
                pltpu.VMEM((DEVS + PAD, 1, hidden + LANES), F32),
                pltpu.VMEM((DEVS + PAD, 1, hidden + LANES), F32),
                pltpu.VMEM((1 + PAD, 1, hidden), F32),
                pltpu.VMEM((DEVS + PAD, 1, hidden), F32),
                pltpu.VMEM((4, DEVS, seq), F32),
                pltpu.VMEM((2, LANES, seq), BF16),
                pltpu.VMEM((slots // DEVS * PART, LANES), jnp.int32),
                pltpu.VMEM((DEVS, hidden), F32),
                pltpu.VMEM((8, LANES), F32),
                pltpu.SemaphoreType.DMA((6,)),
                pltpu.SemaphoreType.DMA((7,)),
                pltpu.SemaphoreType.DMA((7, DEVS // PART)),
            ],
            compiler_params=pltpu.CompilerParams(
                collective_id=0, has_side_effects=True, vmem_limit_bytes=48 * 1024 * 1024),
            name="moe_layer",
        )(x_loc[0], r_loc[0], w_gate.T, w_in_loc[0], w_out_loc[0], first_ids, second_ids, keep_ids)
        loss, gx, dw1, dw2, gw = pl.pallas_call(
            store_kernel,
            out_shape=(
                jax.ShapeDtypeStruct((1, 1), F32),
                jax.ShapeDtypeStruct((seq, hidden), BF16),
                jax.ShapeDtypeStruct((hidden, ff), BF16),
                jax.ShapeDtypeStruct((ff, hidden), BF16),
                jax.ShapeDtypeStruct((DEVS, hidden), F32),
            ),
            in_specs=[vmem] * 9,
            out_specs=(anyspace,) * 5,
            scratch_shapes=[
                pltpu.VMEM((seq, hidden), BF16),
                pltpu.VMEM((late, hidden, wide), BF16),
                pltpu.SMEM((1, 1), F32),
                pltpu.SemaphoreType.DMA((4 + ff // wide,)),
            ],
            compiler_params=pltpu.CompilerParams(vmem_limit_bytes=12 * 1024 * 1024),
            name="store_results",
        )(*results)
        return loss.reshape(()), gx[None], dw1[None], dw2[None], gw.T

    row_spec = P('ep', None, None)
    id_spec = P('ep', None)
    return jax.shard_map(layer_body, mesh=mesh, in_specs=(row_spec, row_spec, P(None, None), row_spec, row_spec, id_spec, id_spec, id_spec), out_specs=(P(), row_spec, row_spec, row_spec, P(None, None)), check_vma=False)
```
